512 devices in a mesh: cx: 16 (over z_hi, y), cy: 32 (over x, z_lo, core).
Axes of the slice: x: 4, y: 8, z: 8 (z_hi: 2, z_lo: 4; z = z_hi * 4 + z_lo), core: 2. Of those that a mesh axis runs over, the one named last changes fastest.
Arguments:
- queries: bfloat16 [7, 32768, 128], P(None, ('cx', 'cy')), may hold values from -8 to 8, as said below
- keys: bfloat16 [32768, 128], P(('cx', 'cy')), may hold values from -40 to 40, as said below
- values: bfloat16 [32768, 128], P(('cx', 'cy')), may hold values from -6 to 6
Outputs:
- attended: bfloat16 [7, 32768, 128], P(None, ('cx', 'cy'))
The draws below stay inside these ranges and needn't reach their ends.
Inputs may be any that keep to these rules, and one draw needn't show every extreme that they name: `queries`: every query is noise of about unit size in each entry plus one common direction of length 4, the same for all heads and tokens. The keys of the first four prompt positions carry a large component along the queries' common direction, so they draw much of every query's attention; all other keys are noise of about unit size in each entry.
All inputs are finite; a program needn't handle non-finite values.
Results may differ from the reference program's by a relative error of at most 0.001.
Values may be sent and summed in bfloat16 or wider, within the bound.
No kernel may reach another device: no remote copies, remote signals or barrier semaphores. Data moves between devices by JAX's collectives and lax.ppermute only.
A program may use at most 192 MiB of HBM per device.

```python
import math
import jax
import jax.numpy as jnp
from jax import lax

HEAD = 128
GROUP = 7
TOK_DEV = 64
SEQ = 32768


def sink_direction(key):
    sample = jax.random.normal(jax.random.fold_in(key, 3), (HEAD,), jnp.float32)
    return sample / jnp.sqrt(jnp.sum(sample * sample))


def noise_field(key, shape):
    return jnp.clip(jax.random.normal(key, shape, jnp.float32), -4.0, 4.0)


def draw_queries(key, part):
    direction = sink_direction(key)
    noise = noise_field(jax.random.fold_in(key, 1), (GROUP, SEQ, HEAD))
    return (noise + 4.0 * direction).astype(jnp.bfloat16)


def draw_keys(key, part):
    direction = sink_direction(key)
    noise = noise_field(jax.random.fold_in(key, 2), (SEQ, HEAD))
    lift = math.sqrt(HEAD) * (math.log(SEQ) - 1.0) / 4.0
    sinks = (jnp.arange(SEQ) < 4).astype(jnp.float32)
    return (noise + lift * sinks[:, None] * direction[None, :]).astype(jnp.bfloat16)


def block_scale(own_key, dims, shards, least, top_value):
    def one(position, parts):
        heights = jax.random.uniform(jax.random.fold_in(jax.random.fold_in(own_key, 6), position), (parts,), jnp.float32, least / len(shards), top_value / len(shards))
        return jnp.repeat(jnp.exp(heights), dims[position] // parts).reshape((-1,) + (1,) * (len(dims) - position - 1))

    level = one(*shards[0])
    for cut in shards[1:]:
        level = level * one(*cut)
    return level


def normal_values(rng, shape, spread, reach, pieces=(), kind=jnp.bfloat16):
    values = spread * jax.random.normal(rng, shape, jnp.float32)
    if pieces:
        values = values * block_scale(rng, shape, pieces, -0.22, 0.18)
    return jnp.clip(values, -reach, reach).astype(kind)


def setup_inputs(seed: int = 0) -> dict:
    key_of = jax.random.split(jax.random.key(seed), 4)
    return {
        "queries": draw_queries(jax.random.fold_in(key_of[3], 71), 0),
        "keys": draw_keys(jax.random.fold_in(key_of[3], 71), 0),
        "values": normal_values(key_of[2], (SEQ, HEAD), 1.0, 6.0, ((0, 512),)),
    }


masked = -1e30


def reference(queries, keys, values):
    key_pos = jnp.arange(SEQ, dtype=jnp.int32)
    values_wide = values.astype(jnp.float32)

    def row_block(number):
        first = (number * TOK_DEV).astype(jnp.int32)
        chosen = lax.dynamic_slice_in_dim(queries, first, TOK_DEV, 1).reshape(GROUP * TOK_DEV, HEAD)
        query_pos = first + jnp.arange(GROUP * TOK_DEV, dtype=jnp.int32) % TOK_DEV
        scores = jnp.dot(chosen, keys.T, preferred_element_type=jnp.float32) * (HEAD ** -0.5)
        visible = key_pos[None, :] <= query_pos[:, None]
        scores = jnp.where(visible, scores, masked)
        peak = jnp.max(scores, axis=1, keepdims=True)
        weights = jnp.where(visible, jnp.exp(scores - peak), 0.0)
        total = jnp.sum(weights, axis=1, keepdims=True)
        mixed = jnp.dot(weights, values_wide, precision=lax.Precision.HIGHEST)
        return (mixed / total).astype(jnp.bfloat16).reshape(GROUP, TOK_DEV, HEAD)

    blocks = lax.map(row_block, jnp.arange(SEQ // TOK_DEV, dtype=jnp.int32))
    return jnp.transpose(blocks, (1, 0, 2, 3)).reshape(GROUP, SEQ, HEAD)
```

```python
import math

import jax
import jax.numpy as jnp
from jax import lax
from jax.experimental import pallas as pl
from jax.experimental.pallas import tpu as pltpu
from jax.sharding import Mesh
from jax.sharding import PartitionSpec as P

AXES = ("zh", "y", "x", "zl", "c")
SIZES = (2, 8, 4, 4, 2)
TEAM = ("x", "c")
Z = ("zh", "zl")

HEAD = 128
GROUP = 7
TOK = 64
ROWS = GROUP * TOK
MATES = 8
SINKS = 4
ALL_ROWS = MATES * ROWS
LANES = 256
STAT = ROWS
EXTRA = STAT + 16 * GROUP
PAYLOAD = EXTRA + 16
masked = -(2.0**100)
SCALE = HEAD**-0.5 * math.log2(math.e)
f32 = jnp.float32
bf16 = jnp.bfloat16


def place():
    return tuple(lax.axis_index(name) for name in AXES)


def attend_kernel(at, q_ref, kv_ref, out_ref, vt_ref):
    zh, y, x, zl, c = (at[i] for i in range(5))
    span = zh * 8 + y
    ones = jnp.ones((16, 256), bf16)

    def turn(tile, carry):
        v = kv_ref[tile // 8, :, tile % 8, :, HEAD:].reshape(256, HEAD)
        vt_ref[tile] = jnp.concatenate([v.astype(f32).T.astype(bf16), ones], axis=0)
        return carry

    lax.fori_loop(0, span + 1, turn, 0)

    def rows_tile(i, carry):
        q = q_ref[pl.ds(pl.multiple_of(i * LANES, LANES), LANES), :]

        def scores_of(tile):
            k = kv_ref[tile // 8, :, tile % 8, :, :HEAD].reshape(256, HEAD)
            return lax.dot_general(k, q, (((1,), (1,)), ((), ())), preferred_element_type=f32) * SCALE

        def fold(tile, state, scores, visible):
            peak, mixed = state
            if visible is not None:
                scores = jnp.where(visible, scores, masked)
            fresh = jnp.maximum(peak, jnp.max(scores, axis=0, keepdims=True))
            weights = jnp.exp2(scores - fresh)
            if visible is not None:
                weights = jnp.where(visible, weights, 0.0)
            update = jnp.dot(vt_ref[tile], weights.astype(bf16), preferred_element_type=f32)
            return fresh, mixed * jnp.exp2(peak - fresh) + update

        def plain(tile, state):
            return fold(tile, state, scores_of(tile), None)

        def edge(tile, state):
            row = i * LANES + lax.broadcasted_iota(jnp.int32, (1, LANES), 1)
            mate = sum((row >= ROWS * n).astype(jnp.int32) for n in range(1, MATES))
            block = span * 32 + (mate >> 1) * 8 + zl * 2 + (mate & 1)
            query_pos = block * TOK + (row & (TOK - 1))
            key = lax.broadcasted_iota(jnp.int32, (256, 1), 0)
            key_pos = (tile * 32 + x * 8 + (key >> 6) * 2 + c) * TOK + (key & (TOK - 1))
            visible = (key_pos <= query_pos) & (key_pos >= SINKS)
            return fold(tile, state, scores_of(tile), visible)

        state = (jnp.full((1, LANES), masked, f32), jnp.zeros((HEAD + 16, LANES), f32))
        state = edge(0, state)
        state = lax.fori_loop(1, span, plain, state)
        state = lax.fori_loop(jnp.maximum(span, 1), span + 1, edge, state)
        peak, mixed = state
        sent = peak.astype(bf16)
        mixed = mixed * jnp.exp2(peak - sent.astype(f32))
        total = mixed[HEAD : HEAD + 1]
        high = total.astype(bf16)
        low = (total - high.astype(f32)).astype(bf16)
        stat = jnp.concatenate([sent, high, low, jnp.zeros((13, LANES), bf16)], axis=0)
        turned = mixed[:HEAD].T.astype(bf16)
        for part in range(LANES // TOK):
            piece = i * (LANES // TOK) + part
            mate = piece // GROUP
            head = piece - mate * GROUP
            out_ref[mate, pl.ds(pl.multiple_of(head * TOK, TOK), TOK), :] = turned[part * TOK : (part + 1) * TOK]
            lanes = slice(part // 2 * 128, part // 2 * 128 + 128)
            out_ref[mate, pl.ds(pl.multiple_of(STAT + head * 16, 16), 16), :] = stat[:, lanes]
        return carry

    lax.fori_loop(0, ALL_ROWS // LANES, rows_tile, 0)
    first = kv_ref[0, 0, 0, :8, :].astype(f32)
    both = jnp.concatenate([first[:SINKS, :HEAD], first[:SINKS, HEAD:], jnp.zeros((8, HEAD), f32)], axis=0).astype(bf16)
    for mate in range(MATES):
        out_ref[mate, EXTRA:, :] = both


def combine_kernel(at, q_ref, got_ref, out_ref, turn_ref):
    zh, y, x, zl, c = (at[i] for i in range(5))
    mate = x * 2 + c
    first = ((zh * 8 + y) * 32 + x * 8 + zl * 2 + c) * TOK
    extra = got_ref[0, EXTRA:, :]
    values = extra.astype(f32)
    for head in range(GROUP):
        q = q_ref[head * TOK : (head + 1) * TOK, :]
        twice = jnp.concatenate([q, q], axis=0)
        scores = lax.dot_general(extra, twice, (((1,), (1,)), ((), ())), preferred_element_type=f32)[:8] * SCALE
        number = lax.broadcasted_iota(jnp.int32, (8, 128), 0)
        token = lax.broadcasted_iota(jnp.int32, (8, 128), 1) & (TOK - 1)
        visible = (number < SINKS) & (number <= first + token)
        scores = jnp.where(visible, scores, masked)
        stats = [got_ref[k, STAT + head * 16 : STAT + head * 16 + 16, :].astype(f32) for k in range(MATES)]
        peaks = jnp.concatenate([s[0:1] for s in stats], axis=0)
        totals = jnp.concatenate([s[1:2] + s[2:3] for s in stats], axis=0)
        peak = jnp.maximum(jnp.max(scores, axis=0, keepdims=True), jnp.max(peaks, axis=0, keepdims=True))
        sinks = jnp.where(visible, jnp.exp2(scores - peak), 0.0)
        shares = jnp.exp2(peaks - peak)
        total = jnp.sum(sinks, axis=0, keepdims=True) + jnp.sum(shares * totals, axis=0, keepdims=True)
        table = jnp.concatenate([shares / total, sinks / total, jnp.zeros((112, 128), f32)], axis=0)
        turn_ref[...] = table.T
        half = pl.multiple_of(((mate + head) & 1) * TOK, TOK)
        factors = turn_ref[pl.ds(half, TOK), :]
        mixed = jnp.zeros((TOK, HEAD), f32)
        for k in range(MATES):
            mixed = mixed + factors[:, k : k + 1] * got_ref[k, head * TOK : (head + 1) * TOK, :].astype(f32)
        for s in range(SINKS):
            mixed = mixed + factors[:, MATES + s : MATES + s + 1] * values[SINKS + s : SINKS + s + 1, :]
        out_ref[head * TOK : (head + 1) * TOK, :] = mixed.astype(bf16)


def everyone(block, axes, count):
    copies = jnp.broadcast_to(block[None], (count, *block.shape))
    return lax.all_to_all(copies, axes, 0, 0, tiled=True)


def per_device(queries, keys, values):
    at = jnp.stack(place()).astype(jnp.int32)
    q = queries.reshape(ROWS, HEAD)
    q_all = lax.all_gather(q, TEAM, axis=0, tiled=True)
    kv = jnp.concatenate([keys, values], axis=1)
    kv = everyone(kv, "y", 8)
    kv = everyone(kv, Z, 8).reshape(2, 4, 8, TOK, 2 * HEAD)
    smem = pl.BlockSpec(memory_space=pltpu.SMEM)
    vmem = pl.BlockSpec(memory_space=pltpu.VMEM)
    partial = pl.pallas_call(
        attend_kernel,
        out_shape=jax.ShapeDtypeStruct((MATES, PAYLOAD, HEAD), bf16),
        in_specs=[smem, vmem, vmem],
        out_specs=vmem,
        scratch_shapes=[pltpu.VMEM((16, HEAD + 16, 256), bf16)],
        name="attend",
    )(at, q_all, kv)
    got = lax.all_to_all(partial, TEAM, 0, 0, tiled=True)
    out = pl.pallas_call(
        combine_kernel,
        out_shape=jax.ShapeDtypeStruct((ROWS, HEAD), bf16),
        in_specs=[smem, vmem, vmem],
        out_specs=vmem,
        scratch_shapes=[pltpu.VMEM((128, 128), f32)],
        name="combine",
    )(at, q, got)
    return out.reshape(GROUP, TOK, HEAD)


def solution(mesh):
    split = Mesh(mesh.devices.reshape(SIZES), AXES)
    shard = P(None, AXES, None)
    return jax.shard_map(
        per_device,
        mesh=split,
        in_specs=(shard, P(AXES, None), P(AXES, None)),
        out_specs=shard,
        check_vma=False,
    )
```

```python
import math

import jax
import jax.numpy as jnp
from jax import lax
from jax.experimental import pallas as pl
from jax.experimental.pallas import tpu as pltpu
from jax.sharding import Mesh
from jax.sharding import PartitionSpec as P

AXES = ("zh", "y", "x", "zl", "c")
SIZES = (2, 8, 4, 4, 2)
TEAM = ("x", "c")
Z = ("zh", "zl")

HEAD = 128
GROUP = 7
TOK = 64
ROWS = GROUP * TOK
MATES = 8
SINKS = 4
ALL_ROWS = MATES * ROWS
STAT = ROWS
CHUNKS = 4
EXTRA = STAT + 16 * CHUNKS
PAYLOAD = EXTRA + 16
masked = -(2.0**100)
SCALE = HEAD**-0.5 * math.log2(math.e)
f32 = jnp.float32
bf16 = jnp.bfloat16


def place():
    return tuple(lax.axis_index(name) for name in AXES)


def attend_kernel(at, q_ref, kv_ref, out_ref, sum_ref, peak_ref):
    zh, y, x, zl, c = (at[i] for i in range(5))
    span = zh * 8 + y

    def keys_of(tile):
        return kv_ref[tile // 8, :, tile % 8, :, :HEAD].reshape(256, HEAD)

    def values_of(tile):
        v = kv_ref[tile // 8, :, tile % 8, :, HEAD:].reshape(256, HEAD)
        return jnp.concatenate([v, jnp.ones((256, HEAD), bf16)], axis=1)

    def rows_of(mate):
        if isinstance(mate, int):
            return slice(mate * ROWS, (mate + 1) * ROWS)
        return pl.ds(pl.multiple_of(mate * ROWS, ROWS), ROWS)

    def scores_of(k, mate):
        q = q_ref[rows_of(mate), :]
        return lax.dot_general(q, k, (((1,), (1,)), ((), ())), preferred_element_type=f32) * SCALE

    def visible_of(tile, mate):
        block = span * 32 + (mate >> 1) * 8 + zl * 2 + (mate & 1)
        query_pos = block * TOK + lax.broadcasted_iota(jnp.int32, (TOK, 1), 0)
        key = lax.broadcasted_iota(jnp.int32, (1, 256), 1)
        key_pos = (tile * 32 + x * 8 + (key >> 6) * 2 + c) * TOK + (key & (TOK - 1))
        return (key_pos <= query_pos) & (key_pos >= SINKS)

    def keep(visible, array, other):
        array = array.reshape(GROUP, TOK, 256)
        return jnp.where(visible[None], array, other).reshape(ROWS, 256)

    def shifted(scores, mate):
        peak = peak_ref[rows_of(mate), :]
        return jnp.exp2(scores - jnp.concatenate([peak] * (scores.shape[1] // HEAD), axis=1))

    def mix(weights, v):
        return jnp.dot(weights.astype(bf16), v, preferred_element_type=f32)

    k, v = keys_of(0), values_of(0)
    for mate in range(MATES):
        visible = visible_of(0, mate)
        scores = keep(visible, scores_of(k, mate), masked)
        peak = jnp.max(scores, axis=1, keepdims=True).astype(bf16).astype(f32)
        peak_ref[rows_of(mate), :] = jnp.broadcast_to(peak, (ROWS, HEAD))
        sum_ref[rows_of(mate), :] = mix(keep(visible, shifted(scores, mate), 0.0), v)

    pairs = jnp.maximum(span - 1, 0) // 2

    def pair(number, carry):
        tile = 1 + 2 * number
        k = jnp.concatenate([keys_of(tile), keys_of(tile + 1)], axis=0)
        v = jnp.concatenate([values_of(tile), values_of(tile + 1)], axis=0)
        for mate in range(MATES):
            sum_ref[rows_of(mate), :] += mix(shifted(scores_of(k, mate), mate), v)
        return carry

    lax.fori_loop(0, pairs, pair, 0)

    def edge(tile, carry):
        k, v = keys_of(tile), values_of(tile)
        for mate in range(MATES):
            weights = shifted(scores_of(k, mate), mate)
            sum_ref[rows_of(mate), :] += mix(keep(visible_of(tile, mate), weights, 0.0), v)
        return carry

    lax.fori_loop(1 + 2 * pairs, span + 1, edge, 0)

    @pl.when(jnp.logical_not(jnp.max(sum_ref[:, HEAD:]) < 2.0**120))
    def _():
        def mate_rows(mate, carry):
            rows = rows_of(mate)
            peak_ref[rows, :] = jnp.full((ROWS, HEAD), masked, f32)
            sum_ref[rows, :] = jnp.zeros((ROWS, 2 * HEAD), f32)

            def step(tile, carry):
                visible = visible_of(tile, mate)
                scores = keep(visible, scores_of(keys_of(tile), mate), masked)
                top = jnp.max(scores, axis=1, keepdims=True)
                old = peak_ref[rows, :]
                peak = jnp.maximum(old, jnp.broadcast_to(top, (ROWS, HEAD)))
                peak_ref[rows, :] = peak
                shrink = jnp.exp2(old - peak)
                fresh = mix(keep(visible, shifted(scores, mate), 0.0), values_of(tile))
                sum_ref[rows, :] = sum_ref[rows, :] * jnp.concatenate([shrink, shrink], axis=1) + fresh
                return carry

            lax.fori_loop(0, span + 1, step, 0)
            peak = peak_ref[rows, :]
            sent = peak.astype(bf16).astype(f32)
            shrink = jnp.exp2(peak - sent)
            peak_ref[rows, :] = sent
            sum_ref[rows, :] = sum_ref[rows, :] * jnp.concatenate([shrink, shrink], axis=1)
            return carry

        lax.fori_loop(0, MATES, mate_rows, 0)

    lane = lax.broadcasted_iota(jnp.int32, (1, HEAD), 1)
    first = kv_ref[0, 0, 0, :8, :].astype(f32)
    both = jnp.concatenate([first[:SINKS, :HEAD], first[:SINKS, HEAD:], jnp.zeros((8, HEAD), f32)], axis=0).astype(bf16)
    for mate in range(MATES):
        out_ref[mate, :ROWS, :] = sum_ref[rows_of(mate), :HEAD].astype(bf16)
        total = sum_ref[rows_of(mate), HEAD:]
        high = total.astype(bf16).astype(f32)
        stat = jnp.where(lane == 0, peak_ref[rows_of(mate), :], jnp.where(lane == 1, high, total - high))
        stat = jnp.concatenate([stat, jnp.zeros((TOK, HEAD), f32)], axis=0)
        for chunk in range(CHUNKS):
            turned = stat[chunk * 128 : (chunk + 1) * 128].T
            out_ref[mate, STAT + 16 * chunk : STAT + 16 * (chunk + 1), :] = turned[:16].astype(bf16)
        out_ref[mate, EXTRA:, :] = both


def combine_kernel(at, q_ref, got_ref, out_ref):
    zh, y, x, zl, c = (at[i] for i in range(5))
    first = ((zh * 8 + y) * 32 + x * 8 + zl * 2 + c) * TOK
    extra = got_ref[0, EXTRA:, :]
    values = extra.astype(f32)
    number = lax.broadcasted_iota(jnp.int32, (8, 128), 0)
    token = lax.broadcasted_iota(jnp.int32, (8, 128), 1) & (TOK - 1)
    visible = (number < SINKS) & (number <= first + token)
    for chunk in range(CHUNKS):
        size = min(128, ROWS - 128 * chunk)
        rows = slice(128 * chunk, 128 * chunk + size)
        q = q_ref[rows, :]
        if size < 128:
            q = jnp.concatenate([q, q], axis=0)
        scores = lax.dot_general(extra, q, (((1,), (1,)), ((), ())), preferred_element_type=f32)[:8] * SCALE
        scores = jnp.where(visible, scores, masked)
        at_row = STAT + 16 * chunk
        stats = [got_ref[k, at_row : at_row + 16, :].astype(f32) for k in range(MATES)]
        peaks = jnp.concatenate([s[0:1] for s in stats], axis=0)
        totals = jnp.concatenate([s[1:2] + s[2:3] for s in stats], axis=0)
        peak = jnp.maximum(jnp.max(scores, axis=0, keepdims=True), jnp.max(peaks, axis=0, keepdims=True))
        sinks = jnp.where(visible, jnp.exp2(scores - peak), 0.0)
        shares = jnp.exp2(peaks - peak)
        total = jnp.sum(sinks, axis=0, keepdims=True) + jnp.sum(shares * totals, axis=0, keepdims=True)
        table = jnp.concatenate([shares / total, sinks / total, jnp.zeros((112, 128), f32)], axis=0)
        factors = table.T[:size]
        mixed = jnp.zeros((size, HEAD), f32)
        for k in range(MATES):
            mixed = mixed + factors[:, k : k + 1] * got_ref[k, rows, :].astype(f32)
        for s in range(SINKS):
            mixed = mixed + factors[:, MATES + s : MATES + s + 1] * values[SINKS + s : SINKS + s + 1, :]
        out_ref[rows, :] = mixed.astype(bf16)


def everyone(block, axes, count):
    copies = jnp.broadcast_to(block[None], (count, *block.shape))
    return lax.all_to_all(copies, axes, 0, 0, tiled=True)


def per_device(queries, keys, values):
    at = jnp.stack(place()).astype(jnp.int32)
    q = queries.reshape(ROWS, HEAD)
    q_all = lax.all_gather(q, TEAM, axis=0, tiled=True)
    kv = jnp.concatenate([keys, values], axis=1)
    kv = everyone(kv, "y", 8)
    kv = everyone(kv, Z, 8).reshape(2, 4, 8, TOK, 2 * HEAD)
    smem = pl.BlockSpec(memory_space=pltpu.SMEM)
    vmem = pl.BlockSpec(memory_space=pltpu.VMEM)
    partial = pl.pallas_call(
        attend_kernel,
        out_shape=jax.ShapeDtypeStruct((MATES, PAYLOAD, HEAD), bf16),
        in_specs=[smem, vmem, vmem],
        out_specs=vmem,
        scratch_shapes=[pltpu.VMEM((ALL_ROWS, 2 * HEAD), f32), pltpu.VMEM((ALL_ROWS, HEAD), f32)],
        name="attend",
    )(at, q_all, kv)
    got = lax.all_to_all(partial, TEAM, 0, 0, tiled=True)
    out = pl.pallas_call(
        combine_kernel,
        out_shape=jax.ShapeDtypeStruct((ROWS, HEAD), bf16),
        in_specs=[smem, vmem, vmem],
        out_specs=vmem,
        name="combine",
    )(at, q, got)
    return out.reshape(GROUP, TOK, HEAD)


def solution(mesh):
    split = Mesh(mesh.devices.reshape(SIZES), AXES)
    shard = P(None, AXES, None)
    return jax.shard_map(
        per_device,
        mesh=split,
        in_specs=(shard, P(AXES, None), P(AXES, None)),
        out_specs=shard,
        check_vma=False,
    )
```

```python
import functools
import math

import jax
import jax.numpy as jnp
from jax import lax
from jax.experimental import pallas as pl
from jax.experimental.pallas import tpu as pltpu
from jax.sharding import Mesh
from jax.sharding import PartitionSpec as P

AXES = ("zh", "y", "x", "zl", "c")
SIZES = (2, 8, 4, 4, 2)
TEAM = ("x", "c")
Z = ("zh", "zl")

HEAD = 128
GROUP = 7
TOK = 64
ROWS = GROUP * TOK
MATES = 8
STEPS = (0, 7, 1, 6, 2, 5, 3)
SINKS = 4
ALL_ROWS = MATES * ROWS
CHUNKS = 4
STAT = ROWS
EXTRA = STAT + 16
PAYLOAD = EXTRA + 16
masked = -(2.0**100)
SCALE = HEAD**-0.5 * math.log2(math.e)
f32 = jnp.float32
bf16 = jnp.bfloat16


def place():
    return tuple(lax.axis_index(name) for name in AXES)


def rows_of(mate):
    if isinstance(mate, int):
        return slice(mate * ROWS, (mate + 1) * ROWS)
    return pl.ds(pl.multiple_of(mate * ROWS, ROWS), ROWS)


def scores_of(q_ref, k, mate):
    q = q_ref[rows_of(mate), :]
    return lax.dot_general(q, k, (((1,), (1,)), ((), ())), preferred_element_type=f32) * SCALE


def positions(at, zk, ys, count):
    zh, y, x, zl, c = at
    key = lax.broadcasted_iota(jnp.int32, (1, count), 1)
    block = ((zk // 4) * 8 + ys + (key >> 6)) * 32 + x * 8 + (zk % 4) * 2 + c
    return block * TOK + (key & (TOK - 1))


def query_positions(at, mate):
    zh, y, x, zl, c = at
    block = (zh * 8 + y) * 32 + (mate >> 1) * 8 + zl * 2 + (mate & 1)
    return block * TOK + lax.broadcasted_iota(jnp.int32, (TOK, 1), 0)


def keep(visible, array, other):
    array = array.reshape(GROUP, TOK, visible.shape[1])
    return jnp.where(visible[None], array, other).reshape(ROWS, visible.shape[1])


def mix(weights, v):
    return jnp.dot(weights.astype(bf16), v, preferred_element_type=f32)


def with_ones(at, v, zk, ys):
    zh, y, x, zl, c = at
    rows = v.shape[0]
    start = ((zk * 8 + ys) * 4 + x) * 2 + c
    row = lax.broadcasted_iota(jnp.int32, (rows, 1), 0)
    v = jnp.concatenate([v, jnp.ones((rows, HEAD), bf16)], axis=1)
    return jnp.where((start > 0) | (row >= SINKS), v.astype(f32), 0.0).astype(bf16)


def fold_pieces(at, q_ref, kv_ref, sum_ref, count, offsets):
    zh, y, x, zl, c = at

    def piece(slot, carry):
        step = offsets[0]
        for n in range(1, count):
            step = jnp.where(slot == n, offsets[n], step)
        zk = (zh * 4 + zl + step) % 8

        @pl.when(zk // 4 < zh)
        def _():
            k = kv_ref[slot, :, :, :HEAD].reshape(512, HEAD)
            v = with_ones(at, kv_ref[slot, :, :, HEAD:].reshape(512, HEAD), zk, 0)
            for mate in range(MATES):
                sum_ref[rows_of(mate), :] += mix(jnp.exp2(scores_of(q_ref, k, mate)), v)

        @pl.when(zk // 4 == zh)
        def _():
            def part(t, carry):
                ys = t * 4
                k = kv_ref[slot, pl.ds(ys, 4), :, :HEAD].reshape(256, HEAD)
                v = with_ones(at, kv_ref[slot, pl.ds(ys, 4), :, HEAD:].reshape(256, HEAD), zk, ys)
                key_pos = positions(at, zk, ys, 256)
                for mate in range(MATES):
                    weights = jnp.exp2(scores_of(q_ref, k, mate))
                    weights = keep(key_pos <= query_positions(at, mate), weights, 0.0)
                    sum_ref[rows_of(mate), :] += mix(weights, v)
                return carry

            lax.fori_loop(0, y // 4 + 1, part, 0)

        return carry

    lax.fori_loop(0, count, piece, 0)


def open_kernel(at_ref, q_ref, own_ref, down_ref, up_ref, sum_ref, kv_ref):
    at = tuple(at_ref[i] for i in range(5))
    kv_ref[0] = own_ref[...]
    kv_ref[1] = down_ref[...]
    kv_ref[2] = up_ref[...]
    sum_ref[...] = jnp.zeros(sum_ref.shape, f32)
    fold_pieces(at, q_ref, kv_ref, sum_ref, 3, (0, 7, 1))


def next_kernel(hops, at_ref, q_ref, down_ref, up_ref, before_ref, sum_ref, kv_ref):
    at = tuple(at_ref[i] for i in range(5))
    kv_ref[0] = down_ref[...]
    kv_ref[1] = up_ref[...]
    fold_pieces(at, q_ref, kv_ref, sum_ref, 2, (8 - hops, hops))


def close_kernel(at_ref, q_ref, down_ref, up_ref, *refs):
    others, (sum_ref, out_ref, kv_ref) = refs[:7], refs[7:]
    at = tuple(at_ref[i] for i in range(5))
    zh, y, x, zl, c = at
    z = zh * 4 + zl
    far = (z + 4) % 8

    @pl.when(far // 4 < zh)
    def _():
        k = jnp.concatenate([ref[:, :, :HEAD].reshape(256, HEAD) for ref in (down_ref, up_ref)], axis=0)
        v = jnp.concatenate([ref[:, :, HEAD:].reshape(256, HEAD) for ref in (down_ref, up_ref)], axis=0)
        v = with_ones(at, v, far, 0)
        for mate in range(MATES):
            sum_ref[rows_of(mate), :] += mix(jnp.exp2(scores_of(q_ref, k, mate)), v)

    lane = lax.broadcasted_iota(jnp.int32, (1, HEAD), 1)
    lowest = jnp.maximum((x * 8 + c) * TOK, SINKS)

    def finish(mate, peak):
        out_ref[mate, :ROWS, :] = sum_ref[rows_of(mate), :HEAD].astype(bf16)
        total = sum_ref[rows_of(mate), HEAD:]
        high = total.astype(bf16).astype(f32)
        stat = jnp.where(lane == 0, peak, jnp.where(lane == 1, high, total - high))
        stat = jnp.concatenate([stat, jnp.zeros((TOK, HEAD), f32)], axis=0)
        tiles = [stat[chunk * 128 : (chunk + 1) * 128].T[:4] for chunk in range(CHUNKS)]
        out_ref[mate, STAT : STAT + 16, :] = jnp.concatenate(tiles, axis=0).astype(bf16)

    lost = jnp.zeros((TOK, HEAD), jnp.bool_)
    for mate in range(MATES):
        total = sum_ref[rows_of(mate), HEAD:].reshape(GROUP, TOK, HEAD)
        seen = query_positions(at, mate) >= lowest
        top = jnp.max(total, axis=0)
        low = jnp.min(total, axis=0)
        lost = lost | jnp.logical_not(top < 2.0**120) | jnp.logical_not((low > 2.0**-40) | jnp.logical_not(seen))
        finish(mate, 0.0)

    @pl.when(jnp.max(jnp.where(lost, 1.0, 0.0)) > 0.0)
    def _():
        for ref, step in zip(others, STEPS):
            kv_ref[(z + step) % 8] = ref[...]
        kv_ref[far, :4] = down_ref[...]
        kv_ref[far, 4:] = up_ref[...]

        def again(mate, carry):
            rows = rows_of(mate)
            sum_ref[rows, :] = jnp.zeros((ROWS, 2 * HEAD), f32)

            def step(tile, peak):
                zk, ys = tile // 2, tile % 2 * 4
                k = kv_ref[zk, pl.ds(ys, 4), :, :HEAD].reshape(256, HEAD)
                v = with_ones(at, kv_ref[zk, pl.ds(ys, 4), :, HEAD:].reshape(256, HEAD), zk, ys)
                key_pos = positions(at, zk, ys, 256)
                visible = (key_pos <= query_positions(at, mate)) & (key_pos >= SINKS)
                scores = keep(visible, scores_of(q_ref, k, mate), masked)
                fresh = jnp.maximum(peak, jnp.max(scores, axis=1, keepdims=True))
                weights = keep(visible, jnp.exp2(scores - fresh), 0.0)
                sum_ref[rows, :] = sum_ref[rows, :] * jnp.exp2(peak - fresh) + mix(weights, v)
                return fresh

            peak = lax.fori_loop(0, 16, step, jnp.full((ROWS, 1), masked, f32))
            sent = peak.astype(bf16).astype(f32)
            sum_ref[rows, :] = sum_ref[rows, :] * jnp.exp2(peak - sent)
            finish(mate, sent)
            return carry

        lax.fori_loop(0, MATES, again, 0)

    both = down_ref[0, :8, :].astype(f32)
    for ref, step in zip(others, STEPS):
        both = jnp.where((z + step) % 8 == 0, ref[0, :8, :].astype(f32), both)
    both = both[:SINKS]
    both = jnp.concatenate([both[:, :HEAD], both[:, HEAD:], jnp.zeros((8, HEAD), f32)], axis=0).astype(bf16)
    for mate in range(MATES):
        out_ref[mate, EXTRA:, :] = both


def combine_kernel(at, q_ref, got_ref, out_ref):
    zh, y, x, zl, c = (at[i] for i in range(5))
    first = ((zh * 8 + y) * 32 + x * 8 + zl * 2 + c) * TOK
    extra = got_ref[0, EXTRA:, :]
    values = extra.astype(f32)
    number = lax.broadcasted_iota(jnp.int32, (8, 128), 0)
    token = lax.broadcasted_iota(jnp.int32, (8, 128), 1) & (TOK - 1)
    visible = (number < SINKS) & (number <= first + token)
    for chunk in range(CHUNKS):
        size = min(128, ROWS - 128 * chunk)
        rows = slice(128 * chunk, 128 * chunk + size)
        q = q_ref[rows, :]
        if size < 128:
            q = jnp.concatenate([q, q], axis=0)
        scores = lax.dot_general(extra, q, (((1,), (1,)), ((), ())), preferred_element_type=f32)[:8] * SCALE
        scores = jnp.where(visible, scores, masked)
        stats = [got_ref[k, STAT : STAT + 16, :].astype(f32)[4 * chunk : 4 * chunk + 4] for k in range(MATES)]
        peaks = jnp.concatenate([s[0:1] for s in stats], axis=0)
        totals = jnp.concatenate([s[1:2] + s[2:3] for s in stats], axis=0)
        peak = jnp.maximum(jnp.max(scores, axis=0, keepdims=True), jnp.max(peaks, axis=0, keepdims=True))
        sinks = jnp.where(visible, jnp.exp2(scores - peak), 0.0)
        shares = jnp.exp2(peaks - peak)
        total = jnp.sum(sinks, axis=0, keepdims=True) + jnp.sum(shares * totals, axis=0, keepdims=True)
        table = jnp.concatenate([shares / total, sinks / total, jnp.zeros((112, 128), f32)], axis=0)
        factors = table.T[:size]
        mixed = jnp.zeros((size, HEAD), f32)
        for k in range(MATES):
            mixed = mixed + factors[:, k : k + 1] * got_ref[k, rows, :].astype(f32)
        for s in range(SINKS):
            mixed = mixed + factors[:, MATES + s : MATES + s + 1] * values[SINKS + s : SINKS + s + 1, :]
        out_ref[rows, :] = mixed.astype(bf16)


def everyone(block, axes, count):
    copies = jnp.broadcast_to(block[None], (count, *block.shape))
    return lax.all_to_all(copies, axes, 0, 0, tiled=True)


def shift(piece, hops):
    return lax.ppermute(piece, Z, [(n, (n + hops) % 8) for n in range(8)])


def cost(keys):
    count = ALL_ROWS * keys
    return pl.CostEstimate(flops=count * 4 * HEAD * 2, transcendentals=count, bytes_accessed=1 << 20)


def per_device(queries, keys, values):
    at = jnp.stack(place()).astype(jnp.int32)
    q = queries.reshape(ROWS, HEAD)
    kv = jnp.concatenate([keys, values], axis=1)
    own = everyone(kv, "y", 8).reshape(8, TOK, 2 * HEAD)
    down1, up1 = shift(own, 1), shift(own, -1)
    q_all = lax.all_gather(q, TEAM, axis=0, tiled=True)
    down2, up2 = shift(down1, 1), shift(up1, -1)
    down3, up3 = shift(down2, 1), shift(up2, -1)
    down4, up4 = shift(down3[:4], 1), shift(up3[4:], -1)
    smem = pl.BlockSpec(memory_space=pltpu.SMEM)
    vmem = pl.BlockSpec(memory_space=pltpu.VMEM)
    roomy = pltpu.CompilerParams(vmem_limit_bytes=32 << 20)
    sums = pltpu.VMEM((ALL_ROWS, 2 * HEAD), f32)
    total = pl.pallas_call(
        open_kernel,
        out_shape=sums,
        in_specs=[smem] + [vmem] * 4,
        out_specs=vmem,
        scratch_shapes=[pltpu.VMEM((3, 8, TOK, 2 * HEAD), bf16)],
        cost_estimate=cost(1536),
        compiler_params=roomy,
        name="open",
    )(at, q_all, own, down1, up1)
    for hops, down, up in ((2, down2, up2), (3, down3, up3)):
        total = pl.pallas_call(
            functools.partial(next_kernel, hops),
            out_shape=sums,
            in_specs=[smem] + [vmem] * 4,
            out_specs=vmem,
            scratch_shapes=[pltpu.VMEM((2, 8, TOK, 2 * HEAD), bf16)],
            input_output_aliases={4: 0},
            cost_estimate=cost(1024),
            compiler_params=roomy,
            name="next%d" % hops,
        )(at, q_all, down, up, total)
    partial = pl.pallas_call(
        close_kernel,
        out_shape=jax.ShapeDtypeStruct((MATES, PAYLOAD, HEAD), bf16),
        in_specs=[smem] + [vmem] * 11,
        out_specs=vmem,
        scratch_shapes=[pltpu.VMEM((8, 8, TOK, 2 * HEAD), bf16)],
        cost_estimate=cost(512),
        compiler_params=roomy,
        name="close",
    )(at, q_all, down4, up4, own, down1, up1, down2, up2, down3, up3, total)
    got = lax.all_to_all(partial, TEAM, 0, 0, tiled=True)
    out = pl.pallas_call(
        combine_kernel,
        out_shape=jax.ShapeDtypeStruct((ROWS, HEAD), bf16),
        in_specs=[smem, vmem, vmem],
        out_specs=vmem,
        name="combine",
    )(at, q, got)
    return out.reshape(GROUP, TOK, HEAD)


def solution(mesh):
    split = Mesh(mesh.devices.reshape(SIZES), AXES)
    shard = P(None, AXES, None)
    return jax.shard_map(
        per_device,
        mesh=split,
        in_specs=(shard, P(AXES, None), P(AXES, None)),
        out_specs=shard,
        check_vma=False,
    )
```

```python
import functools
import math

import jax
import jax.numpy as jnp
from jax import lax
from jax.experimental import pallas as pl
from jax.experimental.pallas import tpu as pltpu
from jax.sharding import Mesh
from jax.sharding import PartitionSpec as P


AXES = ("zh", "y", "x", "zl", "c")
SIZES = (2, 8, 4, 4, 2)
TEAM = ("x", "c")
Z = ("zh", "zl")

HEAD = 128
GROUP = 7
TOK = 64
ROWS = GROUP * TOK
MATES = 8
HOPS = (0, 3, 1, 2)
SEQ = 32768
SINKS = 4
ALL_ROWS = MATES * ROWS
CHUNKS = 4
STAT = ROWS
EXTRA = STAT + 16
PAYLOAD = EXTRA + 16
masked = -(2.0**100)
SCALE = HEAD**-0.5 * math.log2(math.e)
f32 = jnp.float32
bf16 = jnp.bfloat16


def place():
    return tuple(lax.axis_index(name) for name in AXES)


def rows_of(mate):
    if isinstance(mate, int):
        return slice(mate * ROWS, (mate + 1) * ROWS)
    return pl.ds(pl.multiple_of(mate * ROWS, ROWS), ROWS)


def queries_of(q_refs, mate):
    return q_refs[mate // 2][rows_of(mate % 2), :]


def scores_of(q, k):
    return lax.dot_general(q, k, (((1,), (1,)), ((), ())), preferred_element_type=f32) * SCALE


def number_of(at, mate):
    hop = HOPS[mate // 2] if isinstance(mate, int) else jnp.where(mate < 2, 0, jnp.where(mate < 4, 3, jnp.where(mate < 6, 1, 2)))
    return (at[2] + hop) % 4 * 2 + mate % 2


def positions(at, zk, ys, lane, count):
    key = lax.broadcasted_iota(jnp.int32, (1, count), 1)
    block = ((zk // 4) * 8 + ys + (key >> 6)) * 32 + at[2] * 8 + (zk % 4) * 2 + lane
    return block * TOK + (key & (TOK - 1))


def query_positions(at, mate):
    zh, y, _, zl, _ = at
    number = number_of(at, mate)
    block = (zh * 8 + y) * 32 + (number // 2) * 8 + zl * 2 + number % 2
    return block * TOK + lax.broadcasted_iota(jnp.int32, (TOK, 1), 0)


def keep(visible, array, other):
    array = array.reshape(GROUP, TOK, visible.shape[1])
    return jnp.where(visible[None], array, other).reshape(ROWS, visible.shape[1])


def mix(weights, v):
    return jnp.dot(weights.astype(bf16), v, preferred_element_type=f32)


def with_ones(at, v, zk, ys, lane):
    rows = v.shape[0]
    start = ((zk * 8 + ys) * 4 + at[2]) * 2 + lane
    row = lax.broadcasted_iota(jnp.int32, (rows, 1), 0)
    v = jnp.concatenate([v, jnp.ones((rows, HEAD), bf16)], axis=1)
    return jnp.where((start > 0) | (row >= SINKS), v.astype(f32), 0.0).astype(bf16)


def keys_at(ref, lane, ys):
    return ref[lane, pl.ds(ys, 4), :, :HEAD].reshape(256, HEAD)


def values_at(ref, lane, ys):
    return ref[lane, pl.ds(ys, 4), :, HEAD:].reshape(256, HEAD)


def fold_part(at, q_refs, sum_ref, kv_ref, zk, ys, lane):
    k = keys_at(kv_ref, lane, ys)
    v = with_ones(at, values_at(kv_ref, lane, ys), zk, ys, lane)
    key_pos = positions(at, zk, ys, lane, 256)
    for mate in range(MATES):
        weights = jnp.exp2(scores_of(queries_of(q_refs, mate), k))
        weights = keep(key_pos <= query_positions(at, mate), weights, 0.0)
        sum_ref[rows_of(mate), :] += mix(weights, v)


def fold_whole(q_refs, sum_ref, k, v):
    for mate in range(MATES):
        sum_ref[rows_of(mate), :] += mix(jnp.exp2(scores_of(queries_of(q_refs, mate), k)), v)


def fold_piece(at, q_refs, sum_ref, kv_ref, hops):
    zh, y, _, zl, c = at
    zk = (zh * 4 + zl + jnp.where(c == 0, 8 - hops, hops)) % 8

    @pl.when(zk // 4 < zh)
    def _():
        def lane_of(lane, carry):
            k = kv_ref[lane, :, :, :HEAD].reshape(512, HEAD)
            v = with_ones(at, kv_ref[lane, :, :, HEAD:].reshape(512, HEAD), zk, 0, lane)
            fold_whole(q_refs, sum_ref, k, v)
            return carry

        lax.fori_loop(0, 2, lane_of, 0)

    @pl.when(zk // 4 == zh)
    def _():
        def part(n, carry):
            fold_part(at, q_refs, sum_ref, kv_ref, zk, n // 2 * 4, n % 2)
            return carry

        lax.fori_loop(0, (y // 4 + 1) * 2, part, 0)


def half_kernel(at_ref, kv_ref, out_ref):
    out_ref[...] = kv_ref[:, pl.ds(at_ref[4] * 4, 4)]


def open_kernel(at_ref, *refs):
    q_refs, (own_ref, sum_ref) = refs[:4], refs[4:]
    at = zh, y, x, zl, c = tuple(at_ref[i] for i in range(5))
    sum_ref[...] = jnp.zeros(sum_ref.shape, f32)

    @pl.when(c * 4 <= y)
    def _():
        def part(lane, carry):
            fold_part(at, q_refs, sum_ref, own_ref, zh * 4 + zl, c * 4, lane)
            return carry

        lax.fori_loop(0, 2, part, 0)


def next_kernel(hops, at_ref, *refs):
    q_refs, (kv_ref, before_ref, sum_ref) = refs[:4], refs[4:]
    at = tuple(at_ref[i] for i in range(5))
    if hops not in (1, 2, 3):
        sum_ref[...] = before_ref[...]
    fold_piece(at, q_refs, sum_ref, kv_ref, hops)


def close_kernel(at_ref, *refs):
    q_refs, pieces, (far_ref, sum_ref, out_ref, kv_ref, q_copy) = refs[:4], refs[4:8], refs[8:]
    at = zh, y, x, zl, c = tuple(at_ref[i] for i in range(5))
    z = zh * 4 + zl
    far = (z + 4) % 8
    half = c * 4

    @pl.when(far // 4 < zh)
    def _():
        k = far_ref[:, :, :, :HEAD].reshape(512, HEAD)
        v = [with_ones(at, far_ref[lane, :, :, HEAD:].reshape(256, HEAD), far, half, lane) for lane in range(2)]
        fold_whole(q_refs, sum_ref, k, jnp.concatenate(v, axis=0))

    number_row = lax.broadcasted_iota(jnp.int32, (1, HEAD), 1)
    where_z = [(z + jnp.where(c == 0, 8 - n, n)) % 8 for n in range(5)]
    first_y = [half, 0, 0, 0, half]
    lowest = SEQ
    for zk, ys in zip(where_z, first_y):
        lowest = jnp.minimum(lowest, ((zk // 4 * 8 + ys) * 32 + x * 8 + zk % 4 * 2) * TOK)
    lowest = jnp.maximum(lowest, SINKS)

    def finish(mate, peak):
        number = number_of(at, mate)
        out_ref[number, :ROWS, :] = sum_ref[rows_of(mate), :HEAD].astype(bf16)
        total = sum_ref[rows_of(mate), HEAD:]
        high = total.astype(bf16).astype(f32)
        stat = jnp.where(number_row == 0, peak, jnp.where(number_row == 1, high, total - high))
        stat = jnp.concatenate([stat, jnp.zeros((TOK, HEAD), f32)], axis=0)
        tiles = [stat[chunk * 128 : (chunk + 1) * 128].T[:4] for chunk in range(CHUNKS)]
        out_ref[number, STAT : STAT + 16, :] = jnp.concatenate(tiles, axis=0).astype(bf16)

    lost = jnp.zeros((TOK, HEAD), jnp.bool_)
    for mate in range(MATES):
        total = sum_ref[rows_of(mate), HEAD:].reshape(GROUP, TOK, HEAD)
        seen = query_positions(at, mate) >= lowest
        top = jnp.max(total, axis=0)
        low = jnp.min(total, axis=0)
        lost = lost | jnp.logical_not(top < 2.0**120) | jnp.logical_not((low > 2.0**-40) | jnp.logical_not(seen))
        finish(mate, 0.0)

    @pl.when(jnp.max(jnp.where(lost, 1.0, 0.0)) > 0.0)
    def _():
        for n in range(4):
            kv_ref[n] = pieces[n][...]
            q_copy[2 * n * ROWS : 2 * (n + 1) * ROWS, :] = q_refs[n][...]
        kv_ref[4, :, :4] = far_ref[...]
        kv_ref[4, :, 4:] = far_ref[...]

        def again(mate, carry):
            rows = rows_of(mate)
            sum_ref[rows, :] = jnp.zeros((ROWS, 2 * HEAD), f32)

            def step(tile, peak):
                n, lane, ys = tile // 4, tile // 2 % 2, tile % 2 * 4
                zk = (z + jnp.where(c == 0, 8 - n, n)) % 8
                k = keys_at(kv_ref.at[n], lane, ys)
                v = with_ones(at, values_at(kv_ref.at[n], lane, ys), zk, ys, lane)
                key_pos = positions(at, zk, ys, lane, 256)
                mine = jnp.where((n == 0) | (n == 4), jnp.where(ys == half, 0, SEQ), 0)
                visible = (key_pos + mine <= query_positions(at, mate)) & (key_pos >= SINKS)
                scores = keep(visible, scores_of(q_copy[rows, :], k), masked)
                fresh = jnp.maximum(peak, jnp.max(scores, axis=1, keepdims=True))
                weights = keep(visible, jnp.exp2(scores - fresh), 0.0)
                sum_ref[rows, :] = sum_ref[rows, :] * jnp.exp2(peak - fresh) + mix(weights, v)
                return fresh

            peak = lax.fori_loop(0, 20, step, jnp.full((ROWS, 1), masked, f32))
            sent = peak.astype(bf16).astype(f32)
            sum_ref[rows, :] = sum_ref[rows, :] * jnp.exp2(peak - sent)
            finish(mate, sent)
            return carry

        lax.fori_loop(0, MATES, again, 0)

    both = far_ref[0, 0, :8, :].astype(f32)
    for n in range(4):
        both = jnp.where(where_z[n] == 0, pieces[n][0, 0, :8, :].astype(f32), both)
    both = both[:SINKS]
    both = jnp.concatenate([both[:, :HEAD], both[:, HEAD:], jnp.zeros((8, HEAD), f32)], axis=0).astype(bf16)
    for mate in range(MATES):
        out_ref[mate, EXTRA:, :] = both


def combine_kernel(at, q_ref, got_ref, out_ref):
    zh, y, x, zl, c = (at[i] for i in range(5))
    first = ((zh * 8 + y) * 32 + x * 8 + zl * 2 + c) * TOK
    extra = got_ref[jnp.where(zh * 4 + zl <= 4, 0, 1), EXTRA:, :]
    values = extra.astype(f32)
    number = lax.broadcasted_iota(jnp.int32, (8, 128), 0)
    token = lax.broadcasted_iota(jnp.int32, (8, 128), 1) & (TOK - 1)
    visible = (number < SINKS) & (number <= first + token)
    for chunk in range(CHUNKS):
        size = min(128, ROWS - 128 * chunk)
        rows = slice(128 * chunk, 128 * chunk + size)
        q = q_ref[rows, :]
        if size < 128:
            q = jnp.concatenate([q, q], axis=0)
        scores = lax.dot_general(extra, q, (((1,), (1,)), ((), ())), preferred_element_type=f32)[:8] * SCALE
        scores = jnp.where(visible, scores, masked)
        stats = [got_ref[k, STAT : STAT + 16, :].astype(f32)[4 * chunk : 4 * chunk + 4] for k in range(MATES)]
        peaks = jnp.concatenate([s[0:1] for s in stats], axis=0)
        totals = jnp.concatenate([s[1:2] + s[2:3] for s in stats], axis=0)
        peak = jnp.maximum(jnp.max(scores, axis=0, keepdims=True), jnp.max(peaks, axis=0, keepdims=True))
        sinks = jnp.where(visible, jnp.exp2(scores - peak), 0.0)
        shares = jnp.exp2(peaks - peak)
        total = jnp.sum(sinks, axis=0, keepdims=True) + jnp.sum(shares * totals, axis=0, keepdims=True)
        table = jnp.concatenate([shares / total, sinks / total, jnp.zeros((112, 128), f32)], axis=0)
        factors = table.T[:size]
        mixed = jnp.zeros((size, HEAD), f32)
        for k in range(MATES):
            mixed = mixed + factors[:, k : k + 1] * got_ref[k, rows, :].astype(f32)
        for s in range(SINKS):
            mixed = mixed + factors[:, MATES + s : MATES + s + 1] * values[SINKS + s : SINKS + s + 1, :]
        out_ref[rows, :] = mixed.astype(bf16)


def onward(piece):
    pairs = [(2 * z, (2 * z + 2) % 16) for z in range(8)] + [(2 * z + 1, (2 * z + 15) % 16) for z in range(8)]
    return lax.ppermute(piece, (*Z, "c"), pairs)


def along_x(block, hops):
    return lax.ppermute(block, "x", [(n, (n + hops) % 4) for n in range(4)])


def cost(keys):
    count = ALL_ROWS * keys
    return pl.CostEstimate(flops=count * 4 * HEAD * 2, transcendentals=count, bytes_accessed=1 << 20)


def per_device(queries, keys, values):
    at = jnp.stack(place()).astype(jnp.int32)
    q = queries.reshape(ROWS, HEAD)
    q_own = lax.all_gather(q, "c", axis=0, tiled=True)
    kv = jnp.broadcast_to(jnp.concatenate([keys, values], axis=1)[None], (8, TOK, 2 * HEAD))
    own = lax.all_to_all(kv, "y", 0, 0, tiled=True)
    q_all = [q_own]
    for hops in (1, -1, 2):
        q_all.append(along_x(q_own, hops))
    own = lax.all_gather(own, "c", axis=0)
    smem = pl.BlockSpec(memory_space=pltpu.SMEM)
    vmem = pl.BlockSpec(memory_space=pltpu.VMEM)
    piece1 = onward(own)
    piece2 = onward(piece1)
    piece3 = onward(piece2)
    part = pl.pallas_call(
        half_kernel,
        out_shape=pltpu.VMEM((2, 4, TOK, 2 * HEAD), bf16),
        in_specs=[smem, vmem],
        out_specs=vmem,
        compiler_params=pltpu.CompilerParams(vmem_limit_bytes=4 << 20),
        name="half",
    )(at, piece3)
    far = onward(part)
    roomy = pltpu.CompilerParams(vmem_limit_bytes=32 << 20)
    sums = pltpu.VMEM((ALL_ROWS, 2 * HEAD), f32)
    total = pl.pallas_call(
        open_kernel,
        out_shape=sums,
        in_specs=[smem] + [vmem] * 5,
        out_specs=vmem,
        cost_estimate=cost(512),
        compiler_params=roomy,
        name="open",
    )(at, *q_all, own)
    for hops, piece in ((1, piece1), (2, piece2), (3, piece3)):
        total = pl.pallas_call(
            functools.partial(next_kernel, hops),
            out_shape=sums,
            in_specs=[smem] + [vmem] * 6,
            out_specs=vmem,
            input_output_aliases={6: 0} if hops in (1, 2, 3) else {},
            cost_estimate=cost(1024),
            compiler_params=roomy,
        )(at, *q_all, piece, total)
    partial = pl.pallas_call(
        close_kernel,
        out_shape=jax.ShapeDtypeStruct((MATES, PAYLOAD, HEAD), bf16),
        in_specs=[smem] + [vmem] * 10,
        out_specs=vmem,
        scratch_shapes=[pltpu.VMEM((5, 2, 8, TOK, 2 * HEAD), bf16), pltpu.VMEM((ALL_ROWS, HEAD), bf16)],
        cost_estimate=cost(512),
        compiler_params=roomy,
        name="close",
    )(at, *q_all, own, piece1, piece2, piece3, far, total)
    got = lax.all_to_all(partial, TEAM, 0, 0, tiled=True)
    out = pl.pallas_call(
        combine_kernel,
        out_shape=jax.ShapeDtypeStruct((ROWS, HEAD), bf16),
        in_specs=[smem, vmem, vmem],
        out_specs=vmem,
        compiler_params=roomy,
        name="combine",
    )(at, q, got)
    return out.reshape(GROUP, TOK, HEAD)


def solution(mesh):
    split = Mesh(mesh.devices.reshape(SIZES), AXES)
    shard = P(None, AXES, None)
    return jax.shard_map(
        per_device,
        mesh=split,
        in_specs=(shard, P(AXES, None), P(AXES, None)),
        out_specs=shard,
        check_vma=False,
    )
```

```python
import functools
import math

import jax
import jax.numpy as jnp
from jax import lax
from jax.experimental import pallas as pl
from jax.experimental.pallas import tpu as pltpu
from jax.sharding import Mesh
from jax.sharding import PartitionSpec as P


AXES = ("zh", "y", "x", "zl", "c")
SIZES = (2, 8, 4, 4, 2)
TEAM = ("x", "c")
Z = ("zh", "zl")

HEAD = 128
GROUP = 7
TOK = 64
ROWS = GROUP * TOK
MATES = 8
HOPS = (0, 3, 1, 2)
SEQ = 32768
SINKS = 4
ALL_ROWS = MATES * ROWS
CHUNKS = 4
STAT = ROWS
EXTRA = STAT + 16
PAYLOAD = EXTRA + 16
masked = -(2.0**100)
SCALE = HEAD**-0.5 * math.log2(math.e)
f32 = jnp.float32
bf16 = jnp.bfloat16


def place():
    return tuple(lax.axis_index(name) for name in AXES)


def rows_of(mate):
    if isinstance(mate, int):
        return slice(mate * ROWS, (mate + 1) * ROWS)
    return pl.ds(pl.multiple_of(mate * ROWS, ROWS), ROWS)


def queries_of(q_refs, mate):
    return q_refs[mate // 2][rows_of(mate % 2), :]


def scores_of(q, k):
    return lax.dot_general(q, k, (((1,), (1,)), ((), ())), preferred_element_type=f32) * SCALE


def number_of(at, mate):
    hop = HOPS[mate // 2] if isinstance(mate, int) else jnp.where(mate < 2, 0, jnp.where(mate < 4, 3, jnp.where(mate < 6, 1, 2)))
    return (at[2] + hop) % 4 * 2 + mate % 2


def positions(at, zk, ys, lane, count):
    key = lax.broadcasted_iota(jnp.int32, (1, count), 1)
    block = ((zk // 4) * 8 + ys + (key >> 6)) * 32 + at[2] * 8 + (zk % 4) * 2 + lane
    return block * TOK + (key & (TOK - 1))


def query_positions(at, mate):
    zh, y, _, zl, _ = at
    number = number_of(at, mate)
    block = (zh * 8 + y) * 32 + (number // 2) * 8 + zl * 2 + number % 2
    return block * TOK + lax.broadcasted_iota(jnp.int32, (TOK, 1), 0)


def keep(visible, array, other):
    array = array.reshape(GROUP, TOK, visible.shape[1])
    return jnp.where(visible[None], array, other).reshape(ROWS, visible.shape[1])


def mix(weights, v):
    return jnp.dot(weights.astype(bf16), v, preferred_element_type=f32)


def with_ones(at, v, zk, ys, lane):
    rows = v.shape[0]
    start = ((zk * 8 + ys) * 4 + at[2]) * 2 + lane
    row = lax.broadcasted_iota(jnp.int32, (rows, 1), 0)
    v = jnp.concatenate([v, jnp.ones((rows, HEAD), bf16)], axis=1)
    return jnp.where((start > 0) | (row >= SINKS), v.astype(f32), 0.0).astype(bf16)


def keys_at(ref, lane, ys):
    return ref[lane, pl.ds(ys, 4), :, :HEAD].reshape(256, HEAD)


def values_at(ref, lane, ys):
    return ref[lane, pl.ds(ys, 4), :, HEAD:].reshape(256, HEAD)


def fold_part(at, q_refs, sum_ref, kv_ref, zk, ys, lane):
    k = keys_at(kv_ref, lane, ys)
    v = with_ones(at, values_at(kv_ref, lane, ys), zk, ys, lane)
    key_pos = positions(at, zk, ys, lane, 256)
    for mate in range(MATES):
        weights = jnp.exp2(scores_of(queries_of(q_refs, mate), k))
        weights = keep(key_pos <= query_positions(at, mate), weights, 0.0)
        sum_ref[rows_of(mate), :] += mix(weights, v)


def fold_whole(q_refs, sum_ref, k, v):
    for mate in range(MATES):
        sum_ref[rows_of(mate), :] += mix(jnp.exp2(scores_of(queries_of(q_refs, mate), k)), v)


def fold_piece(at, q_refs, sum_ref, kv_ref, hops):
    zh, y, _, zl, c = at
    zk = (zh * 4 + zl + jnp.where(c == 0, 8 - hops, hops)) % 8

    @pl.when(zk // 4 < zh)
    def _():
        def lane_of(lane, carry):
            k = kv_ref[lane, :, :, :HEAD].reshape(512, HEAD)
            v = with_ones(at, kv_ref[lane, :, :, HEAD:].reshape(512, HEAD), zk, 0, lane)
            fold_whole(q_refs, sum_ref, k, v)
            return carry

        lax.fori_loop(0, 2, lane_of, 0)

    @pl.when(zk // 4 == zh)
    def _():
        def part(n, carry):
            fold_part(at, q_refs, sum_ref, kv_ref, zk, n // 2 * 4, n % 2)
            return carry

        lax.fori_loop(0, (y // 4 + 1) * 2, part, 0)


def open_kernel(at_ref, *refs):
    q_refs, (own_ref, sum_ref, kv_ref) = refs[:4], refs[4:]
    at = zh, y, x, zl, c = tuple(at_ref[i] for i in range(5))
    kv_ref[c] = own_ref[...]
    sum_ref[...] = jnp.zeros(sum_ref.shape, f32)

    def part(n, carry):
        fold_part(at, q_refs, sum_ref, kv_ref, zh * 4 + zl, n * 4, c)
        return carry

    lax.fori_loop(0, y // 4 + 1, part, 0)


def next_kernel(hops, at_ref, *refs):
    q_refs, (mine_ref, other_ref, before_ref, sum_ref, kv_ref) = refs[:4], refs[4:]
    at = tuple(at_ref[i] for i in range(5))
    kv_ref[at[4]] = mine_ref[...]
    kv_ref[1 - at[4]] = other_ref[...]
    fold_piece(at, q_refs, sum_ref, kv_ref, hops)


def close_kernel(at_ref, *refs):
    q_refs, mines, others, (sum_ref, out_ref, kv_ref, q_copy) = refs[:4], refs[4:9], refs[9:12], refs[12:]
    far_ref = mines[4]
    at = zh, y, x, zl, c = tuple(at_ref[i] for i in range(5))
    z = zh * 4 + zl
    far = (z + 4) % 8

    @pl.when(far // 4 < zh)
    def _():
        k = far_ref[:, :, :HEAD].reshape(512, HEAD)
        v = with_ones(at, far_ref[:, :, HEAD:].reshape(512, HEAD), far, 0, c)
        fold_whole(q_refs, sum_ref, k, v)

    number_row = lax.broadcasted_iota(jnp.int32, (1, HEAD), 1)
    where_z = [(z + jnp.where(c == 0, 8 - n, n)) % 8 for n in range(5)]
    lowest = SEQ
    for zk, lane in zip(where_z, (c, 0, 0, 0, c)):
        lowest = jnp.minimum(lowest, (zk // 4 * 256 + x * 8 + zk % 4 * 2 + lane) * TOK)
    lowest = jnp.maximum(lowest, SINKS)

    def finish(mate, peak):
        number = number_of(at, mate)
        out_ref[number, :ROWS, :] = sum_ref[rows_of(mate), :HEAD].astype(bf16)
        total = sum_ref[rows_of(mate), HEAD:]
        high = total.astype(bf16).astype(f32)
        stat = jnp.where(number_row == 0, peak, jnp.where(number_row == 1, high, total - high))
        stat = jnp.concatenate([stat, jnp.zeros((TOK, HEAD), f32)], axis=0)
        tiles = [stat[chunk * 128 : (chunk + 1) * 128].T[:4] for chunk in range(CHUNKS)]
        out_ref[number, STAT : STAT + 16, :] = jnp.concatenate(tiles, axis=0).astype(bf16)

    lost = jnp.zeros((TOK, HEAD), jnp.bool_)
    for mate in range(MATES):
        total = sum_ref[rows_of(mate), HEAD:].reshape(GROUP, TOK, HEAD)
        seen = query_positions(at, mate) >= lowest
        top = jnp.max(total, axis=0)
        low = jnp.min(total, axis=0)
        lost = lost | jnp.logical_not(top < 2.0**120) | jnp.logical_not((low > 2.0**-40) | jnp.logical_not(seen))
        finish(mate, 0.0)

    @pl.when(jnp.max(jnp.where(lost, 1.0, 0.0)) > 0.0)
    def _():
        for n in range(5):
            kv_ref[n, c] = mines[n][...]
            kv_ref[n, 1 - c] = others[n - 1][...] if 0 < n < 4 else mines[n][...]
        for n in range(4):
            q_copy[2 * n * ROWS : 2 * (n + 1) * ROWS, :] = q_refs[n][...]

        def again(mate, carry):
            rows = rows_of(mate)
            sum_ref[rows, :] = jnp.zeros((ROWS, 2 * HEAD), f32)

            def step(tile, peak):
                n, lane, ys = tile // 4, tile // 2 % 2, tile % 2 * 4
                zk = (z + jnp.where(c == 0, 8 - n, n)) % 8
                k = keys_at(kv_ref.at[n], lane, ys)
                v = with_ones(at, values_at(kv_ref.at[n], lane, ys), zk, ys, lane)
                key_pos = positions(at, zk, ys, lane, 256)
                mine = jnp.where((n == 0) | (n == 4), jnp.where(lane == c, 0, SEQ), 0)
                visible = (key_pos + mine <= query_positions(at, mate)) & (key_pos >= SINKS)
                scores = keep(visible, scores_of(q_copy[rows, :], k), masked)
                fresh = jnp.maximum(peak, jnp.max(scores, axis=1, keepdims=True))
                weights = keep(visible, jnp.exp2(scores - fresh), 0.0)
                sum_ref[rows, :] = sum_ref[rows, :] * jnp.exp2(peak - fresh) + mix(weights, v)
                return fresh

            peak = lax.fori_loop(0, 20, step, jnp.full((ROWS, 1), masked, f32))
            sent = peak.astype(bf16).astype(f32)
            sum_ref[rows, :] = sum_ref[rows, :] * jnp.exp2(peak - sent)
            finish(mate, sent)
            return carry

        lax.fori_loop(0, MATES, again, 0)

    both = far_ref[0, :8, :].astype(f32)
    for n in range(4):
        first = mines[n][0, :8, :].astype(f32)
        if n > 0:
            first = jnp.where(c == 0, first, others[n - 1][0, :8, :].astype(f32))
        both = jnp.where(where_z[n] == 0, first, both)
    both = both[:SINKS]
    both = jnp.concatenate([both[:, :HEAD], both[:, HEAD:], jnp.zeros((8, HEAD), f32)], axis=0).astype(bf16)
    for mate in range(MATES):
        out_ref[mate, EXTRA:, :] = both


def combine_kernel(at, q_ref, got_ref, out_ref):
    zh, y, x, zl, c = (at[i] for i in range(5))
    first = ((zh * 8 + y) * 32 + x * 8 + zl * 2 + c) * TOK
    extra = got_ref[jnp.where(zh * 4 + zl <= 4, 0, 1), EXTRA:, :]
    values = extra.astype(f32)
    number = lax.broadcasted_iota(jnp.int32, (8, 128), 0)
    token = lax.broadcasted_iota(jnp.int32, (8, 128), 1) & (TOK - 1)
    visible = (number < SINKS) & (number <= first + token)
    for chunk in range(CHUNKS):
        size = min(128, ROWS - 128 * chunk)
        rows = slice(128 * chunk, 128 * chunk + size)
        q = q_ref[rows, :]
        if size < 128:
            q = jnp.concatenate([q, q], axis=0)
        scores = lax.dot_general(extra, q, (((1,), (1,)), ((), ())), preferred_element_type=f32)[:8] * SCALE
        scores = jnp.where(visible, scores, masked)
        stats = [got_ref[k, STAT : STAT + 16, :].astype(f32)[4 * chunk : 4 * chunk + 4] for k in range(MATES)]
        peaks = jnp.concatenate([s[0:1] for s in stats], axis=0)
        totals = jnp.concatenate([s[1:2] + s[2:3] for s in stats], axis=0)
        peak = jnp.maximum(jnp.max(scores, axis=0, keepdims=True), jnp.max(peaks, axis=0, keepdims=True))
        sinks = jnp.where(visible, jnp.exp2(scores - peak), 0.0)
        shares = jnp.exp2(peaks - peak)
        total = jnp.sum(sinks, axis=0, keepdims=True) + jnp.sum(shares * totals, axis=0, keepdims=True)
        table = jnp.concatenate([shares / total, sinks / total, jnp.zeros((112, 128), f32)], axis=0)
        factors = table.T[:size]
        mixed = jnp.zeros((size, HEAD), f32)
        for k in range(MATES):
            mixed = mixed + factors[:, k : k + 1] * got_ref[k, rows, :].astype(f32)
        for s in range(SINKS):
            mixed = mixed + factors[:, MATES + s : MATES + s + 1] * values[SINKS + s : SINKS + s + 1, :]
        out_ref[rows, :] = mixed.astype(bf16)


def onward(piece):
    pairs = [(2 * z, (2 * z + 2) % 16) for z in range(8)] + [(2 * z + 1, (2 * z + 15) % 16) for z in range(8)]
    return lax.ppermute(piece, (*Z, "c"), pairs)


def along_x(block, hops):
    return lax.ppermute(block, "x", [(n, (n + hops) % 4) for n in range(4)])


def cost(keys):
    count = ALL_ROWS * keys
    return pl.CostEstimate(flops=count * 4 * HEAD * 2, transcendentals=count, bytes_accessed=1 << 20)


def per_device(queries, keys, values):
    at = jnp.stack(place()).astype(jnp.int32)
    q = queries.reshape(ROWS, HEAD)
    q_own = lax.all_gather(q, "c", axis=0, tiled=True)
    kv = jnp.broadcast_to(jnp.concatenate([keys, values], axis=1)[None], (8, TOK, 2 * HEAD))
    own = lax.all_to_all(kv, "y", 0, 0, tiled=True)
    q_all = [q_own]
    for hops in (1, -1, 2):
        q_all.append(along_x(q_own, hops))
    smem = pl.BlockSpec(memory_space=pltpu.SMEM)
    vmem = pl.BlockSpec(memory_space=pltpu.VMEM)
    mines = [own]
    for _ in range(1, 5):
        mines.append(onward(mines[-1]))
    others = [lax.ppermute(own, "c", [(0, 1), (1, 0)])]
    for _ in range(1, 4):
        others.append(onward(others[-1]))
    roomy = pltpu.CompilerParams(vmem_limit_bytes=32 << 20)
    sums = pltpu.VMEM((ALL_ROWS, 2 * HEAD), f32)
    total = pl.pallas_call(
        open_kernel,
        out_shape=sums,
        in_specs=[smem] + [vmem] * 5,
        out_specs=vmem,
        scratch_shapes=[pltpu.VMEM((2, 8, TOK, 2 * HEAD), bf16)],
        cost_estimate=cost(512),
        compiler_params=roomy,
        name="open",
    )(at, *q_all, own)
    for hops in (1, 2, 3):
        total = pl.pallas_call(
            functools.partial(next_kernel, hops),
            out_shape=sums,
            in_specs=[smem] + [vmem] * 7,
            out_specs=vmem,
            input_output_aliases={7: 0},
            scratch_shapes=[pltpu.VMEM((2, 8, TOK, 2 * HEAD), bf16)],
            cost_estimate=cost(1024),
            compiler_params=roomy,
        )(at, *q_all, mines[hops], others[hops], total)
    partial = pl.pallas_call(
        close_kernel,
        out_shape=jax.ShapeDtypeStruct((MATES, PAYLOAD, HEAD), bf16),
        in_specs=[smem] + [vmem] * 13,
        out_specs=vmem,
        scratch_shapes=[pltpu.VMEM((5, 2, 8, TOK, 2 * HEAD), bf16), pltpu.VMEM((ALL_ROWS, HEAD), bf16)],
        cost_estimate=cost(512),
        compiler_params=roomy,
        name="close",
    )(at, *q_all, *mines, *others[1:], total)
    got = lax.all_to_all(partial, TEAM, 0, 0, tiled=True)
    out = pl.pallas_call(
        combine_kernel,
        out_shape=jax.ShapeDtypeStruct((ROWS, HEAD), bf16),
        in_specs=[smem, vmem, vmem],
        out_specs=vmem,
        compiler_params=roomy,
        name="combine",
    )(at, q, got)
    return out.reshape(GROUP, TOK, HEAD)


def solution(mesh):
    split = Mesh(mesh.devices.reshape(SIZES), AXES)
    shard = P(None, AXES, None)
    return jax.shard_map(
        per_device,
        mesh=split,
        in_specs=(shard, P(AXES, None), P(AXES, None)),
        out_specs=shard,
        check_vma=False,
    )
```

```python
import functools
import math

import jax
import jax.numpy as jnp
from jax import lax
from jax.experimental import pallas as pl
from jax.experimental.pallas import tpu as pltpu
from jax.sharding import Mesh
from jax.sharding import PartitionSpec as P


AXES = ("zh", "y", "x", "zl", "c")
SIZES = (2, 8, 4, 4, 2)
TEAM = ("x", "c")
Z = ("zh", "zl")

HEAD = 128
GROUP = 7
TOK = 64
ROWS = GROUP * TOK
MATES = 8
HOPS = (0, 3, 1, 2)
SEQ = 32768
SINKS = 4
ALL_ROWS = MATES * ROWS
CHUNKS = 4
STAT = ROWS
EXTRA = STAT + 16
PAYLOAD = EXTRA + 16
masked = -(2.0**100)
SCALE = HEAD**-0.5 * math.log2(math.e)
f32 = jnp.float32
bf16 = jnp.bfloat16


def place():
    return tuple(lax.axis_index(name) for name in AXES)


def rows_of(mate):
    if isinstance(mate, int):
        return slice(mate * ROWS, (mate + 1) * ROWS)
    return pl.ds(pl.multiple_of(mate * ROWS, ROWS), ROWS)


def queries_of(q_refs, mate):
    return q_refs[mate // 2][rows_of(mate % 2), :]


def scores_of(q, k):
    return lax.dot_general(q, k, (((1,), (1,)), ((), ())), preferred_element_type=f32) * SCALE


def number_of(at, mate):
    hop = HOPS[mate // 2] if isinstance(mate, int) else jnp.where(mate < 2, 0, jnp.where(mate < 4, 3, jnp.where(mate < 6, 1, 2)))
    return (at[2] + hop) % 4 * 2 + mate % 2


def positions(at, zk, ys, lane, count):
    key = lax.broadcasted_iota(jnp.int32, (1, count), 1)
    block = ((zk // 4) * 8 + ys + (key >> 6)) * 32 + at[2] * 8 + (zk % 4) * 2 + lane
    return block * TOK + (key & (TOK - 1))


def query_positions(at, mate):
    zh, y, _, zl, _ = at
    number = number_of(at, mate)
    block = (zh * 8 + y) * 32 + (number // 2) * 8 + zl * 2 + number % 2
    return block * TOK + lax.broadcasted_iota(jnp.int32, (TOK, 1), 0)


def keep(visible, array, other):
    array = array.reshape(GROUP, TOK, visible.shape[1])
    return jnp.where(visible[None], array, other).reshape(ROWS, visible.shape[1])


def mix(weights, v):
    return jnp.dot(weights.astype(bf16), v, preferred_element_type=f32)


def with_ones(at, v, zk, ys, lane):
    rows = v.shape[0]
    start = ((zk * 8 + ys) * 4 + at[2]) * 2 + lane
    row = lax.broadcasted_iota(jnp.int32, (rows, 1), 0)
    v = jnp.concatenate([v, jnp.ones((rows, HEAD), bf16)], axis=1)
    return jnp.where((start > 0) | (row >= SINKS), v.astype(f32), 0.0).astype(bf16)


def keys_at(ref, lane, ys):
    return ref[lane, pl.ds(ys, 4), :, :HEAD].reshape(256, HEAD)


def values_at(ref, lane, ys):
    return ref[lane, pl.ds(ys, 4), :, HEAD:].reshape(256, HEAD)


def fold_piece(at, q_refs, sum_ref, kv_ref, zk, lane):
    @pl.when(zk // 4 <= at[0])
    def _():
        k = kv_ref[:, :, :HEAD].reshape(512, HEAD)
        v = with_ones(at, kv_ref[:, :, HEAD:].reshape(512, HEAD), zk, 0, lane)
        key_pos = positions(at, zk, 0, lane, 512)
        for mate in range(MATES):
            weights = jnp.exp2(scores_of(queries_of(q_refs, mate), k))
            weights = keep(key_pos <= query_positions(at, mate), weights, 0.0)
            sum_ref[rows_of(mate), :] += mix(weights, v)


def step_kernel(hops, other, at_ref, *refs):
    q_refs, kv_ref, sum_ref = refs[:4], refs[4], refs[-1]
    at = zh, y, x, zl, c = tuple(at_ref[i] for i in range(5))
    if hops == 0:
        sum_ref[...] = jnp.zeros(sum_ref.shape, f32)
    zk = (zh * 4 + zl + jnp.where(c == 0, 8 - hops, hops)) % 8
    fold_piece(at, q_refs, sum_ref, kv_ref, zk, 1 - c if other else c)


def close_kernel(at_ref, *refs):
    q_refs, mines, others, (sum_ref, out_ref, kv_ref, q_copy) = refs[:4], refs[4:9], refs[9:12], refs[12:]
    far_ref = mines[4]
    at = zh, y, x, zl, c = tuple(at_ref[i] for i in range(5))
    z = zh * 4 + zl
    far = (z + 4) % 8

    fold_piece(at, q_refs, sum_ref, far_ref, far, c)

    number_row = lax.broadcasted_iota(jnp.int32, (1, HEAD), 1)
    where_z = [(z + jnp.where(c == 0, 8 - n, n)) % 8 for n in range(5)]
    lowest = SEQ
    for zk, lane in zip(where_z, (c, 0, 0, 0, c)):
        lowest = jnp.minimum(lowest, (zk // 4 * 256 + x * 8 + zk % 4 * 2 + lane) * TOK)
    lowest = jnp.maximum(lowest, SINKS)

    def finish(mate, peak):
        number = number_of(at, mate)
        out_ref[number, :ROWS, :] = sum_ref[rows_of(mate), :HEAD].astype(bf16)
        total = sum_ref[rows_of(mate), HEAD:]
        high = total.astype(bf16).astype(f32)
        stat = jnp.where(number_row == 0, peak, jnp.where(number_row == 1, high, total - high))
        stat = jnp.concatenate([stat, jnp.zeros((TOK, HEAD), f32)], axis=0)
        tiles = [stat[chunk * 128 : (chunk + 1) * 128].T[:4] for chunk in range(CHUNKS)]
        out_ref[number, STAT : STAT + 16, :] = jnp.concatenate(tiles, axis=0).astype(bf16)

    lost = jnp.zeros((TOK, HEAD), jnp.bool_)
    for mate in range(MATES):
        total = sum_ref[rows_of(mate), HEAD:].reshape(GROUP, TOK, HEAD)
        seen = query_positions(at, mate) >= lowest
        top = jnp.max(total, axis=0)
        low = jnp.min(total, axis=0)
        lost = lost | jnp.logical_not(top < 2.0**120) | jnp.logical_not((low > 2.0**-40) | jnp.logical_not(seen))
        finish(mate, 0.0)

    @pl.when(jnp.max(jnp.where(lost, 1.0, 0.0)) > 0.0)
    def _():
        for n in range(5):
            kv_ref[n, c] = mines[n][...]
            kv_ref[n, 1 - c] = others[n - 1][...] if 0 < n < 4 else mines[n][...]
        for n in range(4):
            q_copy[2 * n * ROWS : 2 * (n + 1) * ROWS, :] = q_refs[n][...]

        def again(mate, carry):
            rows = rows_of(mate)
            sum_ref[rows, :] = jnp.zeros((ROWS, 2 * HEAD), f32)

            def step(tile, peak):
                n, lane, ys = tile // 4, tile // 2 % 2, tile % 2 * 4
                zk = (z + jnp.where(c == 0, 8 - n, n)) % 8
                k = keys_at(kv_ref.at[n], lane, ys)
                v = with_ones(at, values_at(kv_ref.at[n], lane, ys), zk, ys, lane)
                key_pos = positions(at, zk, ys, lane, 256)
                mine = jnp.where((n == 0) | (n == 4), jnp.where(lane == c, 0, SEQ), 0)
                visible = (key_pos + mine <= query_positions(at, mate)) & (key_pos >= SINKS)
                scores = keep(visible, scores_of(q_copy[rows, :], k), masked)
                fresh = jnp.maximum(peak, jnp.max(scores, axis=1, keepdims=True))
                weights = keep(visible, jnp.exp2(scores - fresh), 0.0)
                sum_ref[rows, :] = sum_ref[rows, :] * jnp.exp2(peak - fresh) + mix(weights, v)
                return fresh

            peak = lax.fori_loop(0, 20, step, jnp.full((ROWS, 1), masked, f32))
            sent = peak.astype(bf16).astype(f32)
            sum_ref[rows, :] = sum_ref[rows, :] * jnp.exp2(peak - sent)
            finish(mate, sent)
            return carry

        lax.fori_loop(0, MATES, again, 0)

    both = far_ref[0, :8, :].astype(f32)
    for n in range(4):
        first = mines[n][0, :8, :].astype(f32)
        if n > 0:
            first = jnp.where(c == 0, first, others[n - 1][0, :8, :].astype(f32))
        both = jnp.where(where_z[n] == 0, first, both)
    both = both[:SINKS]
    both = jnp.concatenate([both[:, :HEAD], both[:, HEAD:], jnp.zeros((8, HEAD), f32)], axis=0).astype(bf16)
    for mate in range(MATES):
        out_ref[mate, EXTRA:, :] = both


def combine_kernel(at, q_ref, got_ref, out_ref):
    zh, y, x, zl, c = (at[i] for i in range(5))
    first = ((zh * 8 + y) * 32 + x * 8 + zl * 2 + c) * TOK
    extra = got_ref[jnp.where(zh * 4 + zl <= 4, 0, 1), EXTRA:, :]
    values = extra.astype(f32)
    number = lax.broadcasted_iota(jnp.int32, (8, 128), 0)
    token = lax.broadcasted_iota(jnp.int32, (8, 128), 1) & (TOK - 1)
    visible = (number < SINKS) & (number <= first + token)
    for chunk in range(CHUNKS):
        size = min(128, ROWS - 128 * chunk)
        rows = slice(128 * chunk, 128 * chunk + size)
        q = q_ref[rows, :]
        if size < 128:
            q = jnp.concatenate([q, q], axis=0)
        scores = lax.dot_general(extra, q, (((1,), (1,)), ((), ())), preferred_element_type=f32)[:8] * SCALE
        scores = jnp.where(visible, scores, masked)
        stats = [got_ref[k, STAT : STAT + 16, :].astype(f32)[4 * chunk : 4 * chunk + 4] for k in range(MATES)]
        peaks = jnp.concatenate([s[0:1] for s in stats], axis=0)
        totals = jnp.concatenate([s[1:2] + s[2:3] for s in stats], axis=0)
        peak = jnp.maximum(jnp.max(scores, axis=0, keepdims=True), jnp.max(peaks, axis=0, keepdims=True))
        sinks = jnp.where(visible, jnp.exp2(scores - peak), 0.0)
        shares = jnp.exp2(peaks - peak)
        total = jnp.sum(sinks, axis=0, keepdims=True) + jnp.sum(shares * totals, axis=0, keepdims=True)
        table = jnp.concatenate([shares / total, sinks / total, jnp.zeros((112, 128), f32)], axis=0)
        factors = table.T[:size]
        mixed = jnp.zeros((size, HEAD), f32)
        for k in range(MATES):
            mixed = mixed + factors[:, k : k + 1] * got_ref[k, rows, :].astype(f32)
        for s in range(SINKS):
            mixed = mixed + factors[:, MATES + s : MATES + s + 1] * values[SINKS + s : SINKS + s + 1, :]
        out_ref[rows, :] = mixed.astype(bf16)


def onward(piece):
    pairs = [(2 * z, (2 * z + 2) % 16) for z in range(8)] + [(2 * z + 1, (2 * z + 15) % 16) for z in range(8)]
    return lax.ppermute(piece, (*Z, "c"), pairs)


def along_x(block, hops):
    return lax.ppermute(block, "x", [(n, (n + hops) % 4) for n in range(4)])


def cost(keys):
    count = ALL_ROWS * keys
    return pl.CostEstimate(flops=count * 4 * HEAD * 2, transcendentals=count, bytes_accessed=1 << 20)


def per_device(queries, keys, values):
    at = jnp.stack(place()).astype(jnp.int32)
    q = queries.reshape(ROWS, HEAD)
    q_own = lax.all_gather(q, "c", axis=0, tiled=True)
    kv = jnp.broadcast_to(jnp.concatenate([keys, values], axis=1)[None], (8, TOK, 2 * HEAD))
    own = lax.all_to_all(kv, "y", 0, 0, tiled=True)
    q_all = [q_own]
    for hops in (1, -1, 2):
        q_all.append(along_x(q_own, hops))
    smem = pl.BlockSpec(memory_space=pltpu.SMEM)
    vmem = pl.BlockSpec(memory_space=pltpu.VMEM)
    mines = [own]
    for _ in range(1, 5):
        mines.append(onward(mines[-1]))
    others = [lax.ppermute(own, "c", [(0, 1), (1, 0)])]
    for _ in range(1, 4):
        others.append(onward(others[-1]))
    roomy = pltpu.CompilerParams(vmem_limit_bytes=32 << 20)
    sums = pltpu.VMEM((ALL_ROWS, 2 * HEAD), f32)
    total = ()
    for hops, other in ((0, 0), (1, 0), (1, 1), (2, 0), (2, 1), (3, 0), (3, 1)):
        total = (
            pl.pallas_call(
                functools.partial(step_kernel, hops, other),
                out_shape=sums,
                in_specs=[smem] + [vmem] * (5 + len(total)),
                out_specs=vmem,
                input_output_aliases={6: 0} if total else {},
                cost_estimate=cost(512),
                compiler_params=roomy,
            )(at, *q_all, (others if other else mines)[hops], *total),
        )
    partial = pl.pallas_call(
        close_kernel,
        out_shape=jax.ShapeDtypeStruct((MATES, PAYLOAD, HEAD), bf16),
        in_specs=[smem] + [vmem] * 13,
        out_specs=vmem,
        scratch_shapes=[pltpu.VMEM((5, 2, 8, TOK, 2 * HEAD), bf16), pltpu.VMEM((ALL_ROWS, HEAD), bf16)],
        cost_estimate=cost(512),
        compiler_params=roomy,
        name="close",
    )(at, *q_all, *mines, *others[1:], *total)
    got = lax.all_to_all(partial, TEAM, 0, 0, tiled=True)
    out = pl.pallas_call(
        combine_kernel,
        out_shape=jax.ShapeDtypeStruct((ROWS, HEAD), bf16),
        in_specs=[smem, vmem, vmem],
        out_specs=vmem,
        compiler_params=roomy,
        name="combine",
    )(at, q, got)
    return out.reshape(GROUP, TOK, HEAD)


def solution(mesh):
    split = Mesh(mesh.devices.reshape(SIZES), AXES)
    shard = P(None, AXES, None)
    return jax.shard_map(
        per_device,
        mesh=split,
        in_specs=(shard, P(AXES, None), P(AXES, None)),
        out_specs=shard,
        check_vma=False,
    )
```

```python
import functools
import math

import jax
import jax.numpy as jnp
from jax import lax
from jax.experimental import pallas as pl
from jax.experimental.pallas import tpu as pltpu
from jax.sharding import Mesh
from jax.sharding import PartitionSpec as P


AXES = ("zh", "y", "x", "zl", "c")
SIZES = (2, 8, 4, 4, 2)
TEAM = ("x", "c")
Z = ("zh", "zl")

HEAD = 128
GROUP = 7
TOK = 64
ROWS = GROUP * TOK
MATES = 8
HOPS = (0, 3, 1, 2)
SEQ = 32768
SINKS = 4
ALL_ROWS = MATES * ROWS
CHUNKS = 4
STAT = ROWS
EXTRA = STAT + 16
PAYLOAD = EXTRA + 16
masked = -(2.0**100)
SCALE = HEAD**-0.5 * math.log2(math.e)
f32 = jnp.float32
bf16 = jnp.bfloat16


def place():
    return tuple(lax.axis_index(name) for name in AXES)


def rows_of(mate):
    if isinstance(mate, int):
        return slice(mate * ROWS, (mate + 1) * ROWS)
    return pl.ds(pl.multiple_of(mate * ROWS, ROWS), ROWS)


def queries_of(q_refs, mate):
    return q_refs[mate // 2][rows_of(mate % 2), :]


def scores_of(q, k):
    return lax.dot_general(q, k, (((1,), (1,)), ((), ())), preferred_element_type=f32) * SCALE


def number_of(at, mate):
    hop = HOPS[mate // 2] if isinstance(mate, int) else jnp.where(mate < 2, 0, jnp.where(mate < 4, 3, jnp.where(mate < 6, 1, 2)))
    return (at[2] + hop) % 4 * 2 + mate % 2


def positions(at, zk, ys, lane, count):
    key = lax.broadcasted_iota(jnp.int32, (1, count), 1)
    block = ((zk // 4) * 8 + ys + (key >> 6)) * 32 + at[2] * 8 + (zk % 4) * 2 + lane
    return block * TOK + (key & (TOK - 1))


def query_positions(at, mate):
    zh, y, _, zl, _ = at
    number = number_of(at, mate)
    block = (zh * 8 + y) * 32 + (number // 2) * 8 + zl * 2 + number % 2
    return block * TOK + lax.broadcasted_iota(jnp.int32, (TOK, 1), 0)


def keep(visible, array, other):
    array = array.reshape(GROUP, TOK, visible.shape[1])
    return jnp.where(visible[None], array, other).reshape(ROWS, visible.shape[1])


def mix(weights, v):
    return jnp.dot(weights.astype(bf16), v, preferred_element_type=f32)


def with_ones(at, v, zk, ys, lane):
    rows = v.shape[0]
    start = ((zk * 8 + ys) * 4 + at[2]) * 2 + lane
    row = lax.broadcasted_iota(jnp.int32, (rows, 1), 0)
    v = jnp.concatenate([v, jnp.ones((rows, HEAD), bf16)], axis=1)
    return jnp.where((start > 0) | (row >= SINKS), v.astype(f32), 0.0).astype(bf16)


def keys_at(ref, lane, ys):
    return ref[lane, pl.ds(ys, 4), :, :HEAD].reshape(256, HEAD)


def values_at(ref, lane, ys):
    return ref[lane, pl.ds(ys, 4), :, HEAD:].reshape(256, HEAD)


def fold_piece(at, q_refs, sum_ref, kv_ref, zk, lane, first=False):
    @pl.when(zk // 4 <= at[0])
    def _():
        k = kv_ref[:, :, :HEAD].reshape(512, HEAD)
        v = with_ones(at, kv_ref[:, :, HEAD:].reshape(512, HEAD), zk, 0, lane)
        key_pos = positions(at, zk, 0, lane, 512)
        for mate in range(MATES):
            weights = jnp.exp2(scores_of(queries_of(q_refs, mate), k))
            weights = keep(key_pos <= query_positions(at, mate), weights, 0.0)
            sums = mix(weights, v)
            sum_ref[rows_of(mate), :] = sums if first else sum_ref[rows_of(mate), :] + sums


def step_kernel(hops, other, *refs):
    q_refs, kv_ref, sum_ref = refs[:4], refs[4], refs[-1]
    at = zh, y, x, zl, c = place()
    zk = (zh * 4 + zl + jnp.where(c == 0, 8 - hops, hops)) % 8
    fold_piece(at, q_refs, sum_ref, kv_ref, zk, 1 - c if other else c, first=hops == 0)


def close_kernel(*refs):
    q_refs, mines, others, (sum_ref, out_ref, kv_ref, q_copy) = refs[:4], refs[4:9], refs[9:12], refs[12:]
    far_ref = mines[4]
    at = zh, y, x, zl, c = place()
    z = zh * 4 + zl
    far = (z + 4) % 8

    fold_piece(at, q_refs, sum_ref, far_ref, far, c)

    number_row = lax.broadcasted_iota(jnp.int32, (1, HEAD), 1)
    where_z = [(z + jnp.where(c == 0, 8 - n, n)) % 8 for n in range(5)]
    lowest = SEQ
    for zk, lane in zip(where_z, (c, 0, 0, 0, c)):
        lowest = jnp.minimum(lowest, (zk // 4 * 256 + x * 8 + zk % 4 * 2 + lane) * TOK)
    lowest = jnp.maximum(lowest, SINKS)

    pick = lax.broadcasted_iota(jnp.int32, (16, HEAD), 0) == lax.broadcasted_iota(jnp.int32, (16, HEAD), 1)
    pick = jnp.where(pick, 1.0, 0.0).astype(bf16)

    def finish(mate, peak):
        number = number_of(at, mate)
        out_ref[number, :ROWS, :] = sum_ref[rows_of(mate), :HEAD].astype(bf16)
        total = sum_ref[rows_of(mate), HEAD:]
        high = total.astype(bf16).astype(f32)
        stat = jnp.where(number_row == 0, peak, jnp.where(number_row == 1, high, total - high))
        stat = jnp.where(number_row < 3, stat, 0.0)
        stat = jnp.concatenate([stat, jnp.zeros((TOK, HEAD), f32)], axis=0)
        stat = stat.astype(bf16)
        turned = lax.dot_general(pick, stat, (((1,), (1,)), ((), ())), preferred_element_type=f32)
        tiles = [turned[:4, chunk * 128 : (chunk + 1) * 128] for chunk in range(CHUNKS)]
        out_ref[number, STAT : STAT + 16, :] = jnp.concatenate(tiles, axis=0).astype(bf16)

    lost = jnp.zeros((TOK, HEAD), jnp.bool_)
    for mate in range(MATES):
        total = sum_ref[rows_of(mate), HEAD:].reshape(GROUP, TOK, HEAD)
        seen = query_positions(at, mate) >= lowest
        top = jnp.max(total, axis=0)
        low = jnp.min(total, axis=0)
        lost = lost | jnp.logical_not(top < 2.0**120) | jnp.logical_not((low > 2.0**-40) | jnp.logical_not(seen))
        finish(mate, 0.0)

    @pl.when(jnp.max(jnp.where(lost, 1.0, 0.0)) > 0.0)
    def _():
        for n in range(5):
            kv_ref[n, c] = mines[n][...]
            kv_ref[n, 1 - c] = others[n - 1][...] if 0 < n < 4 else mines[n][...]
        for n in range(4):
            q_copy[2 * n * ROWS : 2 * (n + 1) * ROWS, :] = q_refs[n][...]

        def again(mate, carry):
            rows = rows_of(mate)
            sum_ref[rows, :] = jnp.zeros((ROWS, 2 * HEAD), f32)

            def step(tile, peak):
                n, lane, ys = tile // 4, tile // 2 % 2, tile % 2 * 4
                zk = (z + jnp.where(c == 0, 8 - n, n)) % 8
                k = keys_at(kv_ref.at[n], lane, ys)
                v = with_ones(at, values_at(kv_ref.at[n], lane, ys), zk, ys, lane)
                key_pos = positions(at, zk, ys, lane, 256)
                mine = jnp.where((n == 0) | (n == 4), jnp.where(lane == c, 0, SEQ), 0)
                visible = (key_pos + mine <= query_positions(at, mate)) & (key_pos >= SINKS)
                scores = keep(visible, scores_of(q_copy[rows, :], k), masked)
                fresh = jnp.maximum(peak, jnp.max(scores, axis=1, keepdims=True))
                weights = keep(visible, jnp.exp2(scores - fresh), 0.0)
                sum_ref[rows, :] = sum_ref[rows, :] * jnp.exp2(peak - fresh) + mix(weights, v)
                return fresh

            peak = lax.fori_loop(0, 20, step, jnp.full((ROWS, 1), masked, f32))
            sent = peak.astype(bf16).astype(f32)
            sum_ref[rows, :] = sum_ref[rows, :] * jnp.exp2(peak - sent)
            finish(mate, sent)
            return carry

        lax.fori_loop(0, MATES, again, 0)

    both = far_ref[0, :8, :].astype(f32)
    for n in range(4):
        first = mines[n][0, :8, :].astype(f32)
        if n > 0:
            first = jnp.where(c == 0, first, others[n - 1][0, :8, :].astype(f32))
        both = jnp.where(where_z[n] == 0, first, both)
    both = both[:SINKS]
    both = jnp.concatenate([both[:, :HEAD], both[:, HEAD:], jnp.zeros((8, HEAD), f32)], axis=0).astype(bf16)
    for mate in range(MATES):
        out_ref[mate, EXTRA:, :] = both


def combine_kernel(q_ref, got_ref, out_ref):
    zh, y, x, zl, c = place()
    first = ((zh * 8 + y) * 32 + x * 8 + zl * 2 + c) * TOK
    extra = got_ref[jnp.where(zh * 4 + zl <= 4, 0, 1), EXTRA:, :]
    values = extra.astype(f32)
    number = lax.broadcasted_iota(jnp.int32, (8, 128), 0)
    token = lax.broadcasted_iota(jnp.int32, (8, 128), 1) & (TOK - 1)
    visible = (number < SINKS) & (number <= first + token)
    for chunk in range(CHUNKS):
        size = min(128, ROWS - 128 * chunk)
        rows = slice(128 * chunk, 128 * chunk + size)
        q = q_ref[rows, :]
        if size < 128:
            q = jnp.concatenate([q, q], axis=0)
        scores = lax.dot_general(extra, q, (((1,), (1,)), ((), ())), preferred_element_type=f32)[:8] * SCALE
        scores = jnp.where(visible, scores, masked)
        stats = [got_ref[k, STAT : STAT + 16, :].astype(f32)[4 * chunk : 4 * chunk + 4] for k in range(MATES)]
        peaks = jnp.concatenate([s[0:1] for s in stats], axis=0)
        totals = jnp.concatenate([s[1:2] + s[2:3] for s in stats], axis=0)
        peak = jnp.maximum(jnp.max(scores, axis=0, keepdims=True), jnp.max(peaks, axis=0, keepdims=True))
        sinks = jnp.where(visible, jnp.exp2(scores - peak), 0.0)
        shares = jnp.exp2(peaks - peak)
        total = jnp.sum(sinks, axis=0, keepdims=True) + jnp.sum(shares * totals, axis=0, keepdims=True)
        table = jnp.concatenate([shares / total, sinks / total, jnp.zeros((112, 128), f32)], axis=0)
        factors = table.T[:size]
        mixed = jnp.zeros((size, HEAD), f32)
        for k in range(MATES):
            mixed = mixed + factors[:, k : k + 1] * got_ref[k, rows, :].astype(f32)
        for s in range(SINKS):
            mixed = mixed + factors[:, MATES + s : MATES + s + 1] * values[SINKS + s : SINKS + s + 1, :]
        out_ref[rows, :] = mixed.astype(bf16)


def onward(piece):
    pairs = [(2 * z, (2 * z + 2) % 16) for z in range(8)] + [(2 * z + 1, (2 * z + 15) % 16) for z in range(8)]
    return lax.ppermute(piece, (*Z, "c"), pairs)


def along_x(block, hops):
    return lax.ppermute(block, "x", [(n, (n + hops) % 4) for n in range(4)])


def cost(keys):
    count = ALL_ROWS * keys
    return pl.CostEstimate(flops=count * 4 * HEAD * 2, transcendentals=count, bytes_accessed=1 << 20)


def per_device(queries, keys, values):
    q = queries.reshape(ROWS, HEAD)
    q_own = lax.all_gather(q, "c", axis=0, tiled=True)
    kv = jnp.broadcast_to(jnp.concatenate([keys, values], axis=1)[None], (8, TOK, 2 * HEAD))
    own = lax.all_to_all(kv, "y", 0, 0, tiled=True)
    q_all = [q_own]
    for hops in (1, -1, 2):
        q_all.append(along_x(q_own, hops))
    vmem = pl.BlockSpec(memory_space=pltpu.VMEM)
    mines = [own]
    for _ in range(1, 5):
        mines.append(onward(mines[-1]))
    others = [lax.ppermute(own, "c", [(0, 1), (1, 0)])]
    for _ in range(1, 4):
        others.append(onward(others[-1]))
    roomy = pltpu.CompilerParams(vmem_limit_bytes=32 << 20)
    sums = pltpu.VMEM((ALL_ROWS, 2 * HEAD), f32)
    total = ()
    for hops, other in ((0, 0), (1, 0), (1, 1), (2, 0), (2, 1), (3, 0), (3, 1)):
        total = (
            pl.pallas_call(
                functools.partial(step_kernel, hops, other),
                out_shape=sums,
                in_specs=[vmem] * (5 + len(total)),
                out_specs=vmem,
                input_output_aliases={5: 0} if total else {},
                cost_estimate=cost(512),
                compiler_params=roomy,
            )(*q_all, (others if other else mines)[hops], *total),
        )
    partial = pl.pallas_call(
        close_kernel,
        out_shape=jax.ShapeDtypeStruct((MATES, PAYLOAD, HEAD), bf16),
        in_specs=[vmem] * 13,
        out_specs=vmem,
        scratch_shapes=[pltpu.VMEM((5, 2, 8, TOK, 2 * HEAD), bf16), pltpu.VMEM((ALL_ROWS, HEAD), bf16)],
        cost_estimate=cost(512),
        compiler_params=roomy,
        name="close",
    )(*q_all, *mines, *others[1:], *total)
    got = lax.all_to_all(partial, TEAM, 0, 0, tiled=True)
    out = pl.pallas_call(
        combine_kernel,
        out_shape=jax.ShapeDtypeStruct((ROWS, HEAD), bf16),
        in_specs=[vmem, vmem],
        out_specs=vmem,
        compiler_params=roomy,
        name="combine",
    )(q, got)
    return out.reshape(GROUP, TOK, HEAD)


def solution(mesh):
    split = Mesh(mesh.devices.reshape(SIZES), AXES)
    shard = P(None, AXES, None)
    return jax.shard_map(
        per_device,
        mesh=split,
        in_specs=(shard, P(AXES, None), P(AXES, None)),
        out_specs=shard,
        check_vma=False,
    )
```

```python
import functools
import math

import jax
import jax.numpy as jnp
from jax import lax
from jax.experimental import pallas as pl
from jax.experimental.pallas import tpu as pltpu
from jax.sharding import Mesh
from jax.sharding import PartitionSpec as P


AXES = ("zh", "y", "x", "zl", "c")
SIZES = (2, 8, 4, 4, 2)
TEAM = ("x", "c")
Z = ("zh", "zl")

HEAD = 128
GROUP = 7
TOK = 64
ROWS = GROUP * TOK
MATES = 8
HOPS = (0, 2, 3, 1)
SEQ = 32768
SINKS = 4
ALL_ROWS = MATES * ROWS
CHUNKS = 4
STAT = ROWS
EXTRA = STAT + 16
PAYLOAD = EXTRA + 16
masked = -(2.0**100)
SCALE = HEAD**-0.5 * math.log2(math.e)
f32 = jnp.float32
bf16 = jnp.bfloat16


def place():
    return tuple(lax.axis_index(name) for name in AXES)


def rows_of(mate):
    if isinstance(mate, int):
        return slice(mate * ROWS, (mate + 1) * ROWS)
    return pl.ds(pl.multiple_of(mate * ROWS, ROWS), ROWS)


def queries_of(q_refs, mate):
    return q_refs[mate // 2][rows_of(mate % 2), :]


def scores_of(q, k):
    return lax.dot_general(q, k, (((1,), (1,)), ((), ())), preferred_element_type=f32) * SCALE


def number_of(at, mate):
    hop = HOPS[mate // 2] if isinstance(mate, int) else jnp.where(mate < 2, 0, jnp.where(mate < 4, 2, jnp.where(mate < 6, 3, 1)))
    return (at[2] + hop) % 4 * 2 + mate % 2


def positions(at, zk, ys, lane, count):
    key = lax.broadcasted_iota(jnp.int32, (1, count), 1)
    block = ((zk // 4) * 8 + ys + (key >> 6)) * 32 + at[2] * 8 + (zk % 4) * 2 + lane
    return block * TOK + (key & (TOK - 1))


def query_positions(at, mate):
    zh, y, _, zl, _ = at
    number = number_of(at, mate)
    block = (zh * 8 + y) * 32 + (number // 2) * 8 + zl * 2 + number % 2
    return block * TOK + lax.broadcasted_iota(jnp.int32, (TOK, 1), 0)


def keep(visible, array, other):
    array = array.reshape(GROUP, TOK, visible.shape[1])
    return jnp.where(visible[None], array, other).reshape(ROWS, visible.shape[1])


def mix(weights, v):
    return jnp.dot(weights.astype(bf16), v, preferred_element_type=f32)


def with_ones(at, v, zk, ys, lane):
    rows = v.shape[0]
    start = ((zk * 8 + ys) * 4 + at[2]) * 2 + lane
    row = lax.broadcasted_iota(jnp.int32, (rows, 1), 0)
    v = jnp.concatenate([v, jnp.ones((rows, HEAD), bf16)], axis=1)
    return jnp.where((start > 0) | (row >= SINKS), v.astype(f32), 0.0).astype(bf16)


def keys_at(ref, lane, ys):
    return ref[lane, pl.ds(ys, 4), :, :HEAD].reshape(256, HEAD)


def values_at(ref, lane, ys):
    return ref[lane, pl.ds(ys, 4), :, HEAD:].reshape(256, HEAD)


def fold_piece(at, q_refs, sum_ref, kv_ref, zk, lane, first=False):
    @pl.when(zk // 4 <= at[0])
    def _():
        k = kv_ref[:, :, :HEAD].reshape(512, HEAD)
        v = with_ones(at, kv_ref[:, :, HEAD:].reshape(512, HEAD), zk, 0, lane)
        key_pos = positions(at, zk, 0, lane, 512)
        for mate in range(MATES):
            weights = jnp.exp2(scores_of(queries_of(q_refs, mate), k))
            weights = keep(key_pos <= query_positions(at, mate), weights, 0.0)
            sums = mix(weights, v)
            sum_ref[rows_of(mate), :] = sums if first else sum_ref[rows_of(mate), :] + sums


def step_kernel(hops, other, *refs):
    q_refs, kv_ref, sum_ref = refs[:4], refs[4], refs[-1]
    at = zh, y, x, zl, c = place()
    zk = (zh * 4 + zl + jnp.where(c == 0, 8 - hops, hops)) % 8
    fold_piece(at, q_refs, sum_ref, kv_ref, zk, 1 - c if other else c, first=hops == 0)


def close_kernel(*refs):
    q_refs, mines, others, (sum_ref, out_ref, kv_ref, q_copy) = refs[:4], refs[4:9], refs[9:12], refs[12:]
    far_ref = mines[4]
    at = zh, y, x, zl, c = place()
    z = zh * 4 + zl
    far = (z + 4) % 8

    fold_piece(at, q_refs, sum_ref, far_ref, far, c)

    number_row = lax.broadcasted_iota(jnp.int32, (1, HEAD), 1)
    where_z = [(z + jnp.where(c == 0, 8 - n, n)) % 8 for n in range(5)]
    lowest = SEQ
    for zk, lane in zip(where_z, (c, 0, 0, 0, c)):
        lowest = jnp.minimum(lowest, (zk // 4 * 256 + x * 8 + zk % 4 * 2 + lane) * TOK)
    lowest = jnp.maximum(lowest, SINKS)

    pick = lax.broadcasted_iota(jnp.int32, (16, HEAD), 0) == lax.broadcasted_iota(jnp.int32, (16, HEAD), 1)
    pick = jnp.where(pick, 1.0, 0.0).astype(bf16)

    def finish(mate, peak):
        number = number_of(at, mate)
        out_ref[number, :ROWS, :] = sum_ref[rows_of(mate), :HEAD].astype(bf16)
        total = sum_ref[rows_of(mate), HEAD:]
        high = total.astype(bf16).astype(f32)
        stat = jnp.where(number_row == 0, peak, jnp.where(number_row == 1, high, total - high))
        stat = jnp.where(number_row < 3, stat, 0.0)
        stat = jnp.concatenate([stat, jnp.zeros((TOK, HEAD), f32)], axis=0)
        stat = stat.astype(bf16)
        turned = lax.dot_general(pick, stat, (((1,), (1,)), ((), ())), preferred_element_type=f32)
        tiles = [turned[:4, chunk * 128 : (chunk + 1) * 128] for chunk in range(CHUNKS)]
        out_ref[number, STAT : STAT + 16, :] = jnp.concatenate(tiles, axis=0).astype(bf16)

    lost = jnp.zeros((TOK, HEAD), jnp.bool_)
    for mate in range(MATES):
        total = sum_ref[rows_of(mate), HEAD:].reshape(GROUP, TOK, HEAD)
        seen = query_positions(at, mate) >= lowest
        top = jnp.max(total, axis=0)
        low = jnp.min(total, axis=0)
        lost = lost | jnp.logical_not(top < 2.0**120) | jnp.logical_not((low > 2.0**-40) | jnp.logical_not(seen))
        finish(mate, 0.0)

    @pl.when(jnp.max(jnp.where(lost, 1.0, 0.0)) > 0.0)
    def _():
        for n in range(5):
            kv_ref[n, c] = mines[n][...]
            kv_ref[n, 1 - c] = others[n - 1][...] if 0 < n < 4 else mines[n][...]
        for n in range(4):
            q_copy[2 * n * ROWS : 2 * (n + 1) * ROWS, :] = q_refs[n][...]

        def again(mate, carry):
            rows = rows_of(mate)
            sum_ref[rows, :] = jnp.zeros((ROWS, 2 * HEAD), f32)

            def step(tile, peak):
                n, lane, ys = tile // 4, tile // 2 % 2, tile % 2 * 4
                zk = (z + jnp.where(c == 0, 8 - n, n)) % 8
                k = keys_at(kv_ref.at[n], lane, ys)
                v = with_ones(at, values_at(kv_ref.at[n], lane, ys), zk, ys, lane)
                key_pos = positions(at, zk, ys, lane, 256)
                mine = jnp.where((n == 0) | (n == 4), jnp.where(lane == c, 0, SEQ), 0)
                visible = (key_pos + mine <= query_positions(at, mate)) & (key_pos >= SINKS)
                scores = keep(visible, scores_of(q_copy[rows, :], k), masked)
                fresh = jnp.maximum(peak, jnp.max(scores, axis=1, keepdims=True))
                weights = keep(visible, jnp.exp2(scores - fresh), 0.0)
                sum_ref[rows, :] = sum_ref[rows, :] * jnp.exp2(peak - fresh) + mix(weights, v)
                return fresh

            peak = lax.fori_loop(0, 20, step, jnp.full((ROWS, 1), masked, f32))
            sent = peak.astype(bf16).astype(f32)
            sum_ref[rows, :] = sum_ref[rows, :] * jnp.exp2(peak - sent)
            finish(mate, sent)
            return carry

        lax.fori_loop(0, MATES, again, 0)

    both = far_ref[0, :8, :].astype(f32)
    for n in range(4):
        first = mines[n][0, :8, :].astype(f32)
        if n > 0:
            first = jnp.where(c == 0, first, others[n - 1][0, :8, :].astype(f32))
        both = jnp.where(where_z[n] == 0, first, both)
    both = both[:SINKS]
    both = jnp.concatenate([both[:, :HEAD], both[:, HEAD:], jnp.zeros((8, HEAD), f32)], axis=0).astype(bf16)
    for mate in range(MATES):
        out_ref[mate, EXTRA:, :] = both


def combine_kernel(q_ref, got_ref, out_ref):
    zh, y, x, zl, c = place()
    first = ((zh * 8 + y) * 32 + x * 8 + zl * 2 + c) * TOK
    extra = got_ref[jnp.where(zh * 4 + zl <= 4, 0, 1), EXTRA:, :]
    values = extra.astype(f32)
    number = lax.broadcasted_iota(jnp.int32, (8, 128), 0)
    token = lax.broadcasted_iota(jnp.int32, (8, 128), 1) & (TOK - 1)
    visible = (number < SINKS) & (number <= first + token)
    for chunk in range(CHUNKS):
        size = min(128, ROWS - 128 * chunk)
        rows = slice(128 * chunk, 128 * chunk + size)
        q = q_ref[rows, :]
        if size < 128:
            q = jnp.concatenate([q, q], axis=0)
        scores = lax.dot_general(extra, q, (((1,), (1,)), ((), ())), preferred_element_type=f32)[:8] * SCALE
        scores = jnp.where(visible, scores, masked)
        stats = [got_ref[k, STAT : STAT + 16, :].astype(f32)[4 * chunk : 4 * chunk + 4] for k in range(MATES)]
        peaks = jnp.concatenate([s[0:1] for s in stats], axis=0)
        totals = jnp.concatenate([s[1:2] + s[2:3] for s in stats], axis=0)
        peak = jnp.maximum(jnp.max(scores, axis=0, keepdims=True), jnp.max(peaks, axis=0, keepdims=True))
        sinks = jnp.where(visible, jnp.exp2(scores - peak), 0.0)
        shares = jnp.exp2(peaks - peak)
        total = jnp.sum(sinks, axis=0, keepdims=True) + jnp.sum(shares * totals, axis=0, keepdims=True)
        table = jnp.concatenate([shares / total, sinks / total, jnp.zeros((112, 128), f32)], axis=0)
        factors = table.T[:size]
        mixed = jnp.zeros((size, HEAD), f32)
        for k in range(MATES):
            mixed = mixed + factors[:, k : k + 1] * got_ref[k, rows, :].astype(f32)
        for s in range(SINKS):
            mixed = mixed + factors[:, MATES + s : MATES + s + 1] * values[SINKS + s : SINKS + s + 1, :]
        out_ref[rows, :] = mixed.astype(bf16)


def onward(piece):
    pairs = [(2 * z, (2 * z + 2) % 16) for z in range(8)] + [(2 * z + 1, (2 * z + 15) % 16) for z in range(8)]
    return lax.ppermute(piece, (*Z, "c"), pairs)


def along_x(block, hops):
    return lax.ppermute(block, "x", [(n, (n + hops) % 4) for n in range(4)])


def cost(keys):
    count = ALL_ROWS * keys
    return pl.CostEstimate(flops=count * 4 * HEAD * 2, transcendentals=count, bytes_accessed=1 << 20)


def per_device(queries, keys, values):
    q = queries.reshape(ROWS, HEAD)
    q_own = lax.all_gather(q, "c", axis=0, tiled=True)
    kv = jnp.broadcast_to(jnp.concatenate([keys, values], axis=1)[None], (8, TOK, 2 * HEAD))
    own = lax.all_to_all(kv, "y", 0, 0, tiled=True)
    q_all = [q_own]
    for hops in (2, 1, -1):
        q_all.append(along_x(q_own, hops))
    vmem = pl.BlockSpec(memory_space=pltpu.VMEM)
    mines = [own]
    for _ in range(1, 5):
        mines.append(onward(mines[-1]))
    others = [lax.ppermute(own, "c", [(0, 1), (1, 0)])]
    for _ in range(1, 4):
        others.append(onward(others[-1]))
    roomy = pltpu.CompilerParams(vmem_limit_bytes=32 << 20)
    sums = pltpu.VMEM((ALL_ROWS, 2 * HEAD), f32)
    total = ()
    for hops, other in ((0, 0), (1, 0), (1, 1), (2, 0), (2, 1), (3, 0), (3, 1)):
        total = (
            pl.pallas_call(
                functools.partial(step_kernel, hops, other),
                out_shape=sums,
                in_specs=[vmem] * (5 + len(total)),
                out_specs=vmem,
                input_output_aliases={5: 0} if total else {},
                cost_estimate=cost(512),
                compiler_params=roomy,
            )(*q_all, (others if other else mines)[hops], *total),
        )
    partial = pl.pallas_call(
        close_kernel,
        out_shape=jax.ShapeDtypeStruct((MATES, PAYLOAD, HEAD), bf16),
        in_specs=[vmem] * 13,
        out_specs=vmem,
        scratch_shapes=[pltpu.VMEM((5, 2, 8, TOK, 2 * HEAD), bf16), pltpu.VMEM((ALL_ROWS, HEAD), bf16)],
        cost_estimate=cost(512),
        compiler_params=roomy,
        name="close",
    )(*q_all, *mines, *others[1:], *total)
    got = lax.all_to_all(partial, TEAM, 0, 0, tiled=True)
    out = pl.pallas_call(
        combine_kernel,
        out_shape=jax.ShapeDtypeStruct((ROWS, HEAD), bf16),
        in_specs=[vmem, vmem],
        out_specs=vmem,
        compiler_params=roomy,
        name="combine",
    )(q, got)
    return out.reshape(GROUP, TOK, HEAD)


def solution(mesh):
    split = Mesh(mesh.devices.reshape(SIZES), AXES)
    shard = P(None, AXES, None)
    return jax.shard_map(
        per_device,
        mesh=split,
        in_specs=(shard, P(AXES, None), P(AXES, None)),
        out_specs=shard,
        check_vma=False,
    )
```
